32 devices in a mesh: dp: 4 (over x, core), ctx: 8 (over z, y).
Axes of the slice: x: 2, y: 2, z: 4, core: 2. Of those that a mesh axis runs over, the one named last changes fastest.
Arguments:
- block_input: bfloat16 [4, 1024, 2048], P('dp', 'ctx'), may hold values from -6 to 6
- piece_order: int32 [8, 2], replicated, may hold values from 0 to 15, as said below
- attention_gain: bfloat16 [2048], P(('dp', 'ctx')), may hold values from 0.099609375 to 1.8984375
- query_weight: bfloat16 [2048, 2048], P(('dp', 'ctx')), may hold values from -0.125 to 0.125
- key_matrix: bfloat16 [2048, 512], P(('dp', 'ctx')), may hold values from -0.125 to 0.125
- value_matrix: bfloat16 [2048, 512], P(('dp', 'ctx')), may hold values from -0.125 to 0.125
- output_weight: bfloat16 [2048, 2048], P(('dp', 'ctx')), may hold values from -2 to 2
- feed_gain: bfloat16 [2048], P(('dp', 'ctx')), may hold values from 0.099609375 to 1.8984375
- gate_weight: bfloat16 [2048, 8192], P(('dp', 'ctx')), may hold values from -0.125 to 0.125
- up_weight: bfloat16 [2048, 8192], P(('dp', 'ctx')), may hold values from -0.125 to 0.125
- down_weight: bfloat16 [8192, 2048], P(None, ('dp', 'ctx')), may hold values from -0.0625 to 0.0625
- cotangent: bfloat16 [4, 1024, 2048], P('dp', 'ctx'), may hold values from -6 to 6
Outputs:
- block_output: bfloat16 [4, 1024, 2048], P('dp', 'ctx')
- input_grad: bfloat16 [4, 1024, 2048], P('dp', 'ctx')
- grad_attention_gain: float32 [2048], P(('dp', 'ctx'))
- grad_query: float32 [2048, 2048], P(('dp', 'ctx'))
- grad_key: float32 [2048, 512], P(('dp', 'ctx'))
- grad_value: float32 [2048, 512], P(('dp', 'ctx'))
- grad_output: float32 [2048, 2048], P(('dp', 'ctx'))
- grad_feed_gain: float32 [2048], P(('dp', 'ctx'))
- grad_gate: float32 [2048, 8192], P(('dp', 'ctx'))
- grad_up: float32 [2048, 8192], P(('dp', 'ctx'))
- grad_down: float32 [8192, 2048], P(None, ('dp', 'ctx'))
The draws below stay inside these ranges and needn't reach their ends.
Inputs may be any that keep to these rules, and one draw needn't show every extreme that they name: `piece_order`: each device's two slots hold blocks whose numbers add up to 15, and every block of a sequence is held exactly once.
All inputs are finite; a program needn't handle non-finite values.
Results may differ from the reference program's by a relative error of at most 0.015.
Values may be sent and summed in bfloat16 or wider, within the bound.
A program may use at most 320 MiB of HBM per device.

```python
import math
import jax
import jax.numpy as jnp
from jax import lax

MODEL_DIM = 2048
QUERY_HEADS = 32
KEY_VALUE_HEADS = 8
HEAD_SIZE = 64
FEED_WIDTH = 8192
TOK_DEV = 128
PIECES = 16
SEQUENCE_LENGTH = 1024
SEQS = 4


def draw_piece_order(key, part):
    half_count = PIECES // 2
    order = jax.random.permutation(jax.random.fold_in(key, 11), half_count).astype(jnp.int32)
    partner = (PIECES - 1 - order).astype(jnp.int32)
    flipped = jax.random.randint(jax.random.fold_in(key, 12), (half_count,), 0, 2)
    first_slot = jnp.where(flipped == 1, partner, order)
    second_slot = jnp.where(flipped == 1, order, partner)
    return jnp.stack([first_slot, second_slot], axis=1).astype(jnp.int32)


def strengthened(drawn, stream_key, source, target, parts, factor):
    def block_of(position):
        return (jnp.arange(drawn.shape[position]) // (drawn.shape[position] // parts)).reshape((-1,) + (1,) * (drawn.ndim - 1 - position))

    one_side = jax.random.permutation(stream_key, parts)[block_of(target)]
    second = (block_of(target) + parts // 2) % parts
    return jnp.where((block_of(source) == one_side) | (block_of(source) == second), factor * drawn, drawn)


def block_scale(own_key, dims, split, smallest, high):
    gain = 1.0
    for position, parts in split:
        steps = jax.random.uniform(jax.random.fold_in(jax.random.fold_in(own_key, 6), position), (parts,), jnp.float32, smallest / len(split), high / len(split))
        gain = gain * jnp.repeat(jnp.exp(steps), dims[position] // parts).reshape((-1,) + (1,) * (len(dims) - 1 - position))
    return gain


def centred(stream_key, shape, spread, limit, split=(), kind=jnp.bfloat16):
    level = block_scale(stream_key, shape, split, -0.22, 0.18) if split else 1.0
    result = jax.random.normal(stream_key, shape, jnp.float32) * spread * level
    return jnp.minimum(jnp.maximum(result, -limit), limit).astype(kind)


def heavy_noise(rng, dims, width, bound, split, heavy, kind=jnp.bfloat16):
    values = width * jax.random.normal(rng, dims, jnp.float32)
    if split:
        values = values * block_scale(rng, dims, split, -0.22, 0.18)
    return jnp.clip(strengthened(values, jax.random.fold_in(rng, 3), *heavy), -bound, bound).astype(kind)


def setup_inputs(seed: int = 0) -> dict:
    seeds = jax.random.split(jax.random.key(seed), 13)
    return {
        "block_input": heavy_noise(seeds[0], (SEQS, SEQUENCE_LENGTH, MODEL_DIM), 1.0, 6.0, ((0, 4), (1, 8)), (1, 2, 8, 2.0)),
        "piece_order": draw_piece_order(jax.random.fold_in(seeds[12], 71), 0),
        "attention_gain": jnp.clip(1.0 + 0.18 * jax.random.normal(seeds[2], (MODEL_DIM,), jnp.float32), 0.099609375, 1.8984375).astype(jnp.bfloat16),
        "query_weight": centred(seeds[3], (MODEL_DIM, QUERY_HEADS * HEAD_SIZE), MODEL_DIM ** -0.5, 0.125, ((0, 32),)),
        "key_matrix": centred(seeds[4], (MODEL_DIM, KEY_VALUE_HEADS * HEAD_SIZE), MODEL_DIM ** -0.5, 0.125, ((0, 32),)),
        "value_matrix": centred(seeds[5], (MODEL_DIM, KEY_VALUE_HEADS * HEAD_SIZE), MODEL_DIM ** -0.5, 0.125, ((0, 32),)),
        "output_weight": centred(seeds[6], (QUERY_HEADS * HEAD_SIZE, MODEL_DIM), (max(1, QUERY_HEADS * HEAD_SIZE // 256)) ** -0.5, 2.0, ((0, 32),)),
        "feed_gain": jnp.clip(1.0 + 0.18 * jax.random.normal(seeds[7], (MODEL_DIM,), jnp.float32), 0.099609375, 1.8984375).astype(jnp.bfloat16),
        "gate_weight": centred(seeds[8], (MODEL_DIM, FEED_WIDTH), MODEL_DIM ** -0.5, 0.125, ((0, 32),)),
        "up_weight": centred(seeds[9], (MODEL_DIM, FEED_WIDTH), MODEL_DIM ** -0.5, 0.125, ((0, 32),)),
        "down_weight": centred(seeds[10], (FEED_WIDTH, MODEL_DIM), FEED_WIDTH ** -0.5, 0.0625, ((1, 32),)),
        "cotangent": centred(seeds[11], (SEQS, SEQUENCE_LENGTH, MODEL_DIM), 1.0, 6.0, ((0, 4), (1, 8))),
    }


EPSILON = 1e-05
ROPE_BASE = 500000.0
NEG_FILL = -1e+30

def rounded_values(values):
    return lax.optimization_barrier(values.astype(jnp.bfloat16))

def normalize(rows_in):
    inv_rms = lax.rsqrt(lax.optimization_barrier(jnp.mean(rows_in * rows_in, axis=-1, keepdims=True)) + EPSILON)
    return (rows_in * inv_rms, inv_rms)

def angles(positions, head_dim):
    half_dim = head_dim // 2
    frequency = jnp.exp(jnp.arange(half_dim, dtype=jnp.float32) * (-2.0 * math.log(ROPE_BASE) / head_dim))
    phase_angle = positions.astype(jnp.float32)[:, None] * frequency[None, :]
    return (jnp.cos(phase_angle)[:, None, :], jnp.sin(phase_angle)[:, None, :])

def rotate(tensor, cosine_values, sine_values):
    half_dim = tensor.shape[-1] // 2
    first_half = tensor[..., :half_dim]
    second_half = tensor[..., half_dim:]
    return jnp.concatenate([first_half * cosine_values - second_half * sine_values, second_half * cosine_values + first_half * sine_values], axis=-1)

def inverse_rotate(tensor, cosine_values, sine_values):
    half_dim = tensor.shape[-1] // 2
    first_half = tensor[..., :half_dim]
    second_half = tensor[..., half_dim:]
    return jnp.concatenate([first_half * cosine_values + second_half * sine_values, second_half * cosine_values - first_half * sine_values], axis=-1)

def reference(block_input, piece_order, attention_gain, query_weight, key_matrix, value_matrix, output_weight, feed_gain, gate_weight, up_weight, down_weight, cotangent):
    single_float = jnp.float32
    piece_rows = TOK_DEV // 2
    heads_per_group = QUERY_HEADS // KEY_VALUE_HEADS
    score_scaling = 1.0 / math.sqrt(HEAD_SIZE)
    offsets = jnp.arange(piece_rows, dtype=jnp.int32)
    positions = ((piece_order * piece_rows)[:, :, None] + offsets[None, None, :]).reshape(-1).astype(jnp.int32)
    cosine_values, sine_values = angles(positions, HEAD_SIZE)
    block_length = min(512, SEQUENCE_LENGTH)
    count_of_blocks = SEQUENCE_LENGTH // block_length
    gain_attention = attention_gain.astype(single_float)
    gain_feed = feed_gain.astype(single_float)

    def scores_for(block_queries, pos_block, key_single):
        unscaled_scores = jnp.einsum('whmv,qhv->hmwq', block_queries.astype(single_float), key_single) * score_scaling
        allowed = positions[None, :] <= pos_block[:, None]
        return jnp.where(allowed[None, None], unscaled_scores, NEG_FILL)

    def one_sequence(grad_sums, pair_in):
        rows_in, grad_rows = pair_in
        inputs32 = rows_in.astype(single_float)
        unit_one, inv_one = normalize(inputs32)
        first_normed = rounded_values(unit_one * gain_attention)
        query_heads = jnp.dot(first_normed, query_weight, preferred_element_type=single_float).reshape(SEQUENCE_LENGTH, QUERY_HEADS, HEAD_SIZE)
        heads_of_key = jnp.dot(first_normed, key_matrix, preferred_element_type=single_float).reshape(SEQUENCE_LENGTH, KEY_VALUE_HEADS, HEAD_SIZE)
        heads_of_value = jnp.dot(first_normed, value_matrix, preferred_element_type=single_float).reshape(SEQUENCE_LENGTH, KEY_VALUE_HEADS, HEAD_SIZE)
        rotated_queries = rounded_values(rotate(query_heads, cosine_values, sine_values))
        rotated_keys = rounded_values(rotate(heads_of_key, cosine_values, sine_values))
        block_value_rows = rounded_values(heads_of_value)
        key_single = rotated_keys.astype(single_float)
        value_single = block_value_rows.astype(single_float)
        queries_by_block = rotated_queries.reshape(count_of_blocks, block_length, KEY_VALUE_HEADS, heads_per_group, HEAD_SIZE)
        pos_blocks = positions.reshape(count_of_blocks, block_length)

        def forward_block(pair_block):
            block_queries, pos_block = pair_block
            scores = scores_for(block_queries, pos_block, key_single)
            row_top = lax.optimization_barrier(jnp.max(scores, axis=-1, keepdims=True))
            log_total = row_top[..., 0] + jnp.log(lax.optimization_barrier(jnp.sum(jnp.exp(scores - row_top), axis=-1)))
            softmax_probabilities = rounded_values(jnp.exp(scores - log_total[..., None]))
            block_attended = rounded_values(jnp.einsum('lumo,olf->mluf', softmax_probabilities.astype(single_float), value_single))
            return (block_attended, log_total)
        attended_blocks, log_blocks = lax.map(forward_block, (queries_by_block, pos_blocks))
        attended = attended_blocks.reshape(SEQUENCE_LENGTH, QUERY_HEADS * HEAD_SIZE)
        mid = inputs32 + jnp.dot(attended, output_weight, preferred_element_type=single_float)
        unit_two, inv_two = normalize(mid)
        normed_two = rounded_values(unit_two * gain_feed)
        gate_pre = jnp.dot(normed_two, gate_weight, preferred_element_type=single_float)
        up_pre = jnp.dot(normed_two, up_weight, preferred_element_type=single_float)
        sigmoid_gate = jax.nn.sigmoid(gate_pre)
        swish_gate = gate_pre * sigmoid_gate
        hidden = rounded_values(swish_gate * up_pre)
        block_out = rounded_values(mid + jnp.dot(hidden, down_weight, preferred_element_type=single_float))
        grad_hidden = jnp.dot(grad_rows, down_weight.T, preferred_element_type=single_float)
        grad_gate_pre = rounded_values(grad_hidden * up_pre * sigmoid_gate * (1.0 + gate_pre * (1.0 - sigmoid_gate)))
        grad_up_pre = rounded_values(grad_hidden * swish_gate)
        grad_normed_two = jnp.dot(grad_gate_pre, gate_weight.T, preferred_element_type=single_float) + jnp.dot(grad_up_pre, up_weight.T, preferred_element_type=single_float)
        term_gate = jnp.dot(normed_two.T, grad_gate_pre, preferred_element_type=single_float)
        term_up = jnp.dot(normed_two.T, grad_up_pre, preferred_element_type=single_float)
        term_down = jnp.dot(hidden.T, grad_rows, preferred_element_type=single_float)
        term_feed_gain = lax.optimization_barrier(jnp.sum(grad_normed_two * unit_two, axis=0))
        grad_unit_two = grad_normed_two * gain_feed
        grad_mid = grad_rows.astype(single_float) + inv_two * (grad_unit_two - unit_two * lax.optimization_barrier(jnp.mean(grad_unit_two * unit_two, axis=-1, keepdims=True)))
        grad_mid_b = rounded_values(grad_mid)
        attended_gradient = rounded_values(jnp.dot(grad_mid_b, output_weight.T, preferred_element_type=single_float))
        term_output = jnp.dot(attended.T, grad_mid_b, preferred_element_type=single_float)
        block_gradients = attended_gradient.reshape(count_of_blocks, block_length, KEY_VALUE_HEADS, heads_per_group, HEAD_SIZE)

        def backward_block(key_value_sums, pieces):
            block_queries, pos_block, grad_block, block_attended, log_block = pieces
            scores = scores_for(block_queries, pos_block, key_single)
            softmax_probabilities = jnp.exp(scores - log_block[..., None])
            block_probability = rounded_values(softmax_probabilities)
            gradient_single = grad_block.astype(single_float)
            delta_rows = lax.optimization_barrier(jnp.sum(gradient_single * block_attended.astype(single_float), axis=-1)).transpose(1, 2, 0)
            probability_gradient = jnp.einsum('whmv,qhv->hmwq', gradient_single, value_single)
            score_gradient = rounded_values(softmax_probabilities * (probability_gradient - delta_rows[..., None])).astype(single_float)
            query_block_gradient = jnp.einsum('lumo,olf->mluf', score_gradient, key_single) * score_scaling
            key_gradient_total = key_value_sums[0] + jnp.einsum('hyme,mhyr->ehr', score_gradient, block_queries.astype(single_float)) * score_scaling
            value_gradient_total = key_value_sums[1] + jnp.einsum('hyme,mhyr->ehr', block_probability.astype(single_float), gradient_single)
            return ((key_gradient_total, value_gradient_total), query_block_gradient)
        empty_key_value = jnp.zeros((SEQUENCE_LENGTH, KEY_VALUE_HEADS, HEAD_SIZE), single_float)
        key_value_gradients, grad_query_blocks = lax.scan(backward_block, (empty_key_value, empty_key_value), (queries_by_block, pos_blocks, block_gradients, attended_blocks, log_blocks))
        grad_query_rot = grad_query_blocks.reshape(SEQUENCE_LENGTH, QUERY_HEADS, HEAD_SIZE)
        grad_query_pre = rounded_values(inverse_rotate(grad_query_rot, cosine_values, sine_values)).reshape(SEQUENCE_LENGTH, QUERY_HEADS * HEAD_SIZE)
        key_gradient_before = rounded_values(inverse_rotate(key_value_gradients[0], cosine_values, sine_values)).reshape(SEQUENCE_LENGTH, KEY_VALUE_HEADS * HEAD_SIZE)
        value_gradient_before = rounded_values(key_value_gradients[1]).reshape(SEQUENCE_LENGTH, KEY_VALUE_HEADS * HEAD_SIZE)
        grad_normed_one = jnp.dot(grad_query_pre, query_weight.T, preferred_element_type=single_float) + jnp.dot(key_gradient_before, key_matrix.T, preferred_element_type=single_float) + jnp.dot(value_gradient_before, value_matrix.T, preferred_element_type=single_float)
        term_query = jnp.dot(first_normed.T, grad_query_pre, preferred_element_type=single_float)
        term_key = jnp.dot(first_normed.T, key_gradient_before, preferred_element_type=single_float)
        term_value = jnp.dot(first_normed.T, value_gradient_before, preferred_element_type=single_float)
        term_attention_gain = lax.optimization_barrier(jnp.sum(grad_normed_one * unit_one, axis=0))
        grad_unit_one = grad_normed_one * gain_attention
        grad_input = rounded_values(grad_mid + inv_one * (grad_unit_one - unit_one * lax.optimization_barrier(jnp.mean(grad_unit_one * unit_one, axis=-1, keepdims=True))))
        new_terms = (term_attention_gain, term_query, term_key, term_value, term_output, term_feed_gain, term_gate, term_up, term_down)
        new_sums = tuple((old_sum + new_term for old_sum, new_term in zip(grad_sums, new_terms)))
        return (new_sums, (block_out, grad_input))
    starting_sums = (jnp.zeros((MODEL_DIM,), single_float), jnp.zeros((MODEL_DIM, QUERY_HEADS * HEAD_SIZE), single_float), jnp.zeros((MODEL_DIM, KEY_VALUE_HEADS * HEAD_SIZE), single_float), jnp.zeros((MODEL_DIM, KEY_VALUE_HEADS * HEAD_SIZE), single_float), jnp.zeros((QUERY_HEADS * HEAD_SIZE, MODEL_DIM), single_float), jnp.zeros((MODEL_DIM,), single_float), jnp.zeros((MODEL_DIM, FEED_WIDTH), single_float), jnp.zeros((MODEL_DIM, FEED_WIDTH), single_float), jnp.zeros((FEED_WIDTH, MODEL_DIM), single_float))
    sums, outputs = lax.scan(one_sequence, starting_sums, (block_input, cotangent))
    return (outputs[0], outputs[1], sums[0], sums[1], sums[2], sums[3], sums[4], sums[5], sums[6], sums[7], sums[8])
```

```python
import functools
import math

import jax
import jax.numpy as jnp
from jax import lax
from jax.experimental import pallas as pl
from jax.experimental.pallas import tpu as pltpu
from jax.sharding import PartitionSpec as P

QUERY_HEADS = 32
KEY_VALUE_HEADS = 8
HEAD_SIZE = 64
EPSILON = 1e-05
ROPE_BASE = 500000.0
NEG_FILL = -1e30
ROWS_FIRST = (((0,), (0,)), ((), ()))
LAST_LAST = (((1,), (1,)), ((), ()))
MESH = pl.DeviceIdType.MESH
F32 = jnp.float32
BF16 = jnp.bfloat16
ANY = pl.BlockSpec(memory_space=pl.ANY)
VMEM_LIMIT = 60 * 1024 * 1024


def normalize(rows_in):
    inv_rms = lax.rsqrt(jnp.mean(rows_in * rows_in, axis=-1, keepdims=True) + EPSILON)
    return (rows_in * inv_rms, inv_rms)


def takes(us):
    return pl.CostEstimate(flops=0, bytes_accessed=int(us * 3.5e6), transcendentals=0)


def remote(src, dst, send, recv, dev):
    return pltpu.make_async_remote_copy(
        src_ref=src, dst_ref=dst, send_sem=send, recv_sem=recv, device_id=dev, device_id_type=MESH
    )


class RowGather:
    def __init__(self, n, src, dst, send, send_pair, recv, local):
        self.n, self.nz = n, n // 2
        self.src, self.dst = src, dst
        self.send, self.send_pair, self.recv, self.local = send, send_pair, recv, local
        self.d, self.c = lax.axis_index("dp"), lax.axis_index("ctx")
        self.z, self.y = self.c // 2, lax.rem(self.c, 2)

    def first(self, tz, ty, sem):
        return remote(self.src, self.dst.at[self.c], sem, self.recv.at[self.c], (self.d, tz * 2 + ty))

    def onward(self, s, tz, ty, sem):
        return remote(self.dst.at[s], self.dst.at[s], sem, self.recv.at[s], (self.d, tz * 2 + ty))

    def start(self):
        z, y, nz = self.z, self.y, self.nz
        pltpu.make_async_copy(self.src, self.dst.at[self.c], self.local).start()

        @pl.when(z + 1 < nz)
        def _():
            self.first(z + 1, y, self.send.at[0, 0]).start()

        @pl.when(z > 0)
        def _():
            self.first(z - 1, y, self.send.at[1, 0]).start()

        self.first(z, 1 - y, self.send_pair.at[0]).start()

    def step(self, k):
        z, y, nz = self.z, self.y, self.nz

        @pl.when(z - k >= 0)
        def _():
            s = (z - k) * 2 + y
            self.onward(s, z, y, self.send.at[0, k]).wait_recv()

            @pl.when(z + 1 < nz)
            def _():
                self.onward(s, z + 1, y, self.send.at[0, k]).start()

            self.onward(s, z, 1 - y, self.send_pair.at[k]).start()

        @pl.when(z + k < nz)
        def _():
            s = (z + k) * 2 + y
            self.onward(s, z, y, self.send.at[1, k]).wait_recv()

            @pl.when(z > 0)
            def _():
                self.onward(s, z - 1, y, self.send.at[1, k]).start()

            self.onward(s, z, 1 - y, self.send_pair.at[nz - 1 + k]).start()

    def finish(self):
        z, y, nz = self.z, self.y, self.nz
        pltpu.make_async_copy(self.src, self.dst.at[self.c], self.local).wait()

        def arrived(zz, carry):
            self.onward(zz * 2 + 1 - y, z, y, self.send.at[0, 0]).wait_recv()
            return carry

        lax.fori_loop(0, nz, arrived, 0)
        self.first(z, 1 - y, self.send_pair.at[0]).wait_send()

        @pl.when(z + 1 < nz)
        def _():
            self.first(z + 1, y, self.send.at[0, 0]).wait_send()

        @pl.when(z > 0)
        def _():
            self.first(z - 1, y, self.send.at[1, 0]).wait_send()

        for k in range(1, nz):

            @pl.when(z - k >= 0)
            def _():
                s = (z - k) * 2 + y

                @pl.when(z + 1 < nz)
                def _():
                    self.onward(s, z + 1, y, self.send.at[0, k]).wait_send()

                self.onward(s, z, 1 - y, self.send_pair.at[k]).wait_send()

            @pl.when(z + k < nz)
            def _():
                s = (z + k) * 2 + y

                @pl.when(z > 0)
                def _():
                    self.onward(s, z - 1, y, self.send.at[1, k]).wait_send()

                self.onward(s, z, 1 - y, self.send_pair.at[nz - 1 + k]).wait_send()


class WeightFetch:
    def __init__(self, n, rows, widths, srcs, dsts, out_sem, x_sem, core_sem, recv, local):
        self.n, self.rows, self.widths = n, rows, widths
        self.srcs, self.dsts = srcs, dsts
        self.out_sem, self.x_sem, self.core_sem = out_sem, x_sem, core_sem
        self.recv, self.local = recv, local
        self.d, self.c = lax.axis_index("dp"), lax.axis_index("ctx")
        core = lax.rem(self.d, 2)
        self.d_core = self.d + 1 - 2 * core
        self.d_x = lax.rem(self.d + 2, 4)
        self.items = range(len(srcs))

    def columns(self, i, c):
        w = self.widths[i]
        return self.srcs[i].at[:, pl.ds(pl.multiple_of(c * w, w), w)]

    def block(self, i, r):
        return self.dsts[i].at[pl.ds(pl.multiple_of(r * self.rows, self.rows), self.rows), :]

    def spread(self, i, j):
        t = lax.rem(self.c + j, self.n)
        r = self.d * self.n + self.c
        return remote(
            self.columns(i, t), self.block(i, r), self.out_sem.at[i, j], self.recv.at[i, r], (self.d, t)
        )

    def own_to(self, i, dev_d, sem):
        r = self.d * self.n + self.c
        return remote(self.columns(i, self.c), self.block(i, r), sem, self.recv.at[i, r], (dev_d, self.c))

    def pass_on(self, i, r, dev_d, sem):
        return remote(self.block(i, r), self.block(i, r), sem, self.recv.at[i, r], (dev_d, self.c))

    def own_copy(self, i):
        return pltpu.make_async_copy(
            self.columns(i, self.c), self.block(i, self.d * self.n + self.c), self.local.at[i]
        )

    def start(self):
        for i in self.items:
            self.own_to(i, self.d_x, self.x_sem.at[i, 0]).start()
            self.own_to(i, self.d_core, self.core_sem.at[i, 0]).start()
            self.own_copy(i).start()

        def go(j, carry):
            for i in self.items:
                self.spread(i, j).start()
            return carry

        lax.fori_loop(1, self.n, go, 0)

    def relay(self):
        n = self.n

        def same(j, carry):
            r = self.d * n + lax.rem(self.c + n - j, n)
            for i in self.items:
                self.pass_on(i, r, self.d_x, self.x_sem.at[i, j]).wait_recv()
                self.pass_on(i, r, self.d_x, self.x_sem.at[i, j]).start()
                self.pass_on(i, r, self.d_core, self.core_sem.at[i, j]).start()
            return carry

        lax.fori_loop(1, n, same, 0)

        def across(j, carry):
            r = self.d_x * n + lax.rem(self.c + n - j, n)
            for i in self.items:
                self.pass_on(i, r, self.d_core, self.core_sem.at[i, n + j]).wait_recv()
                self.pass_on(i, r, self.d_core, self.core_sem.at[i, n + j]).start()
            return carry

        lax.fori_loop(0, n, across, 0)

    def finish(self):
        n = self.n
        d_far = lax.rem(self.d_core + 2, 4)
        for i in self.items:
            self.own_copy(i).wait()
            self.own_to(i, self.d_x, self.x_sem.at[i, 0]).wait_send()
            self.own_to(i, self.d_core, self.core_sem.at[i, 0]).wait_send()

        def last(j, carry):
            cc = lax.rem(self.c + n - j, n)
            for i in self.items:
                r = self.d_core * n + cc
                self.pass_on(i, r, self.d_core, self.core_sem.at[i, 0]).wait_recv()
                r = d_far * n + cc
                self.pass_on(i, r, self.d_core, self.core_sem.at[i, 0]).wait_recv()
                r = self.d_x * n + cc
                self.pass_on(i, r, self.d_core, self.core_sem.at[i, n + j]).wait_send()
            return carry

        lax.fori_loop(0, n, last, 0)

        def sent(j, carry):
            r = self.d * n + lax.rem(self.c + n - j, n)
            for i in self.items:
                self.spread(i, j).wait_send()
                self.pass_on(i, r, self.d_x, self.x_sem.at[i, j]).wait_send()
                self.pass_on(i, r, self.d_core, self.core_sem.at[i, j]).wait_send()
            return carry

        lax.fori_loop(1, n, sent, 0)


class OwnerSpread:
    def __init__(self, n, ndp, src, dst, send, recv, local):
        self.ndp, self.src, self.dst = ndp, src, dst
        self.send, self.recv, self.local = send, recv, local
        self.d, self.c = lax.axis_index("dp"), lax.axis_index("ctx")
        me = self.d * n + self.c
        self.target, self.slot = me // ndp, lax.rem(me, ndp)
        self.mine = (self.slot == self.d) & (self.target == self.c)
        self.away = jnp.logical_not(self.mine)

    def first(self):
        return remote(
            self.src, self.dst.at[self.slot], self.send.at[0], self.recv.at[self.slot], (self.slot, self.target)
        )

    def own(self):
        return pltpu.make_async_copy(self.src, self.dst.at[self.d], self.local.at[0])

    def onward(self, k):
        t = lax.rem(self.d + k, self.ndp)
        return remote(self.dst.at[self.d], self.dst.at[self.d], self.send.at[k], self.recv.at[self.d], (t, self.c))

    def back(self, k):
        t = lax.rem(self.d + k, self.ndp)
        return remote(self.dst.at[t], self.dst.at[t], self.send.at[k], self.recv.at[t], (t, self.c))

    def start(self):
        pl.when(self.mine)(lambda: self.own().start())
        pl.when(self.away)(lambda: self.first().start())

    def relay(self):
        pl.when(self.mine)(lambda: self.own().wait())
        pl.when(self.away)(lambda: self.onward(1).wait_recv())
        for k in range(1, self.ndp):
            self.onward(k).start()

    def finish(self):
        pl.when(self.away)(lambda: self.first().wait_send())
        for k in range(1, self.ndp):
            self.onward(k).wait_send()
            self.back(k).wait_recv()


class DpExchange:
    def __init__(self, ndp, srcs, dsts, send, recv, local):
        self.ndp, self.srcs, self.dsts = ndp, srcs, dsts
        self.send, self.recv, self.local = send, recv, local
        self.d, self.c = lax.axis_index("dp"), lax.axis_index("ctx")

    def rows(self, i, j):
        size = self.srcs[i].shape[0] // self.ndp
        return self.srcs[i].at[pl.ds(pl.multiple_of(j * size, size), size), :]

    def copy(self, i, k):
        t = lax.rem(self.d + k, self.ndp)
        return remote(
            self.rows(i, t), self.dsts[i].at[self.d], self.send.at[i, k], self.recv.at[i, self.d], (t, self.c)
        )

    def back(self, i, k):
        t = lax.rem(self.d + k, self.ndp)
        return remote(self.rows(i, t), self.dsts[i].at[t], self.send.at[i, k], self.recv.at[i, t], (t, self.c))

    def own(self, i):
        return pltpu.make_async_copy(self.rows(i, self.d), self.dsts[i].at[self.d], self.local.at[i])

    def start(self):
        for i in range(len(self.srcs)):
            for k in range(1, self.ndp):
                self.copy(i, k).start()
            self.own(i).start()

    def finish(self):
        for i in range(len(self.srcs)):
            for k in range(1, self.ndp):
                self.copy(i, k).wait_send()
                self.back(i, k).wait_recv()
            self.own(i).wait()


def fetch(name, n, ndp, rows_list, weight_list, owned=None):
    count, wcount = len(rows_list), len(weight_list)
    ocount = 0 if owned is None else 1
    arrays = count + wcount + ocount
    widths = [w.shape[1] // n for w in weight_list]
    rows = weight_list[0].shape[0] if weight_list else 0
    total = n * ndp

    def body(*refs):
        ins, rest = refs[:arrays], refs[arrays:]
        outs, sems = rest[:arrays], rest[arrays:]
        gathers = [
            RowGather(n, ins[i], outs[i], sems[0].at[i], sems[1].at[i], sems[2].at[i], sems[3].at[i])
            for i in range(count)
        ]
        for g in gathers:
            g.start()
        weights = None
        if wcount:
            at = slice(count, count + wcount)
            weights = WeightFetch(n, rows, widths, ins[at], outs[at], *sems[4:9])
            weights.start()
        if ocount:
            spread = OwnerSpread(n, ndp, ins[-1], outs[-1], *sems[9:])
            spread.start()
        for k in range(1, n // 2):
            for g in gathers:
                g.step(k)
        if ocount:
            spread.relay()
        if wcount:
            weights.relay()
        for g in gathers:
            g.finish()
        if wcount:
            weights.finish()
        if ocount:
            spread.finish()

    dma = pltpu.SemaphoreType.DMA
    scratch = [
        dma((max(count, 1), 2, n // 2)),
        dma((max(count, 1), n)),
        dma((max(count, 1), n)),
        dma((max(count, 1),)),
    ]
    if wcount:
        scratch += [dma((wcount, n)), dma((wcount, n)), dma((wcount, 2 * n)), dma((wcount, total)), dma((wcount,))]
    outs = [jax.ShapeDtypeStruct((n,) + r.shape, r.dtype) for r in rows_list] + [
        jax.ShapeDtypeStruct((rows * total, w), BF16) for w in widths
    ]
    extra = []
    if ocount:
        scratch += [dma((ndp,)), dma((ndp,)), dma((1,))]
        outs += [jax.ShapeDtypeStruct((ndp,) + owned.shape, BF16)]
        extra = [owned]
    return pl.pallas_call(
        body,
        out_shape=outs,
        in_specs=[ANY] * arrays,
        out_specs=[ANY] * arrays,
        scratch_shapes=scratch,
        name=name,
        cost_estimate=takes(60),
        compiler_params=pltpu.CompilerParams(has_side_effects=True),
    )(*rows_list, *weight_list, *extra)


def turned(blocks, n, axis):
    c = lax.axis_index("ctx")
    order = [blocks[0]] + blocks[:0:-1]
    size = blocks[0].shape[axis]
    double = jnp.concatenate(order + order[:-1], axis=axis)
    return lax.dynamic_slice_in_dim(double, (n - 1 - (c + n - 1) % n) * size, n * size, axis)


def pass_blocks(array, n, axis, join):
    c = lax.axis_index("ctx")
    size = array.shape[axis] // n
    blocks = []
    for j in range(n):
        block = lax.dynamic_slice_in_dim(array, (c + j) % n * size, size, axis)
        if j:
            block = lax.ppermute(block, "ctx", [(i, (i + j) % n) for i in range(n)])
        blocks.append(block)
    return turned(blocks, n, join)


def scatter_sum(name, n, parts, ndp=1, shared=()):
    count, scount = len(parts), len(shared)
    _, rows, width = parts[0].shape
    nz = n // 2
    step_rows = 32

    def body(*refs):
        every = count + scount
        ins, outs = refs[:count], refs[every : every + count]
        own, pair, far, s_own, s_pair, r_pair, s_far, r_far = refs[2 * every : 2 * every + 8]
        exchange = None
        if scount:
            exchange = DpExchange(
                ndp, refs[count:every], refs[every + count : 2 * every], *refs[2 * every + 8 :]
            )
        d, c = lax.axis_index("dp"), lax.axis_index("ctx")
        z, y = c // 2, lax.rem(c, 2)

        def load(a, zz):
            return pltpu.make_async_copy(ins[a].at[zz * 2 + y], own.at[a, zz], s_own.at[a, zz])

        def across(a, zz):
            return remote(
                ins[a].at[zz * 2 + 1 - y], pair.at[a, zz], s_pair.at[a, zz], r_pair.at[a, zz], (d, z * 2 + 1 - y)
            )

        def along(a, zz, tz, slot):
            return remote(pair.at[a, zz], far.at[a, slot], s_far.at[a, zz], r_far.at[a, slot], (d, tz * 2 + y))

        def order(fn):
            for k in range(nz - 1, 0, -1):
                for a in range(count):

                    @pl.when(z - k >= 0)
                    def _():
                        fn(a, z - k, -1)

                    @pl.when(z + k < nz)
                    def _():
                        fn(a, z + k, 1)

            for a in range(count):
                fn(a, z, 0)

        def begin(a, zz, way):
            load(a, zz).start()
            across(a, zz).start()

        order(begin)
        if scount:
            exchange.start()

        def add(a, zz, slots, out):
            def chunk(i, carry):
                at = pl.ds(pl.multiple_of(i * step_rows, step_rows), step_rows)
                total = own[a, zz, at, :].astype(F32) + pair[a, zz, at, :].astype(F32)
                for slot in slots:
                    total = total + far[a, slot, at, :].astype(F32)
                if out is None:
                    pair[a, zz, at, :] = total.astype(BF16)
                else:
                    out[at, :] = total
                return carry

            lax.fori_loop(0, rows // step_rows, chunk, 0)

        def handle(a, zz, way):
            load(a, zz).wait()
            across(a, zz).wait_recv()
            if way == 0:

                @pl.when(z > 0)
                def _():
                    along(a, z, z, z).wait_recv()

                @pl.when(z + 1 < nz)
                def _():
                    along(a, z, z, nz).wait_recv()

                @pl.when(z == 0)
                def _():
                    add(a, z, (nz,), outs[a])

                @pl.when(z + 1 == nz)
                def _():
                    add(a, z, (z,), outs[a])

                @pl.when((z > 0) & (z + 1 < nz))
                def _():
                    add(a, z, (z, nz), outs[a])

                return
            behind = z - way
            has = (behind >= 0) & (behind < nz)

            @pl.when(has)
            def _():
                along(a, zz, z, zz).wait_recv()
                add(a, zz, (zz,), None)

            @pl.when(jnp.logical_not(has))
            def _():
                add(a, zz, (), None)

            tz = z + way
            if way < 0:

                @pl.when(tz == zz)
                def _():
                    along(a, zz, tz, nz).start()

                @pl.when(tz != zz)
                def _():
                    along(a, zz, tz, zz).start()

            else:
                along(a, zz, tz, zz).start()

        order(handle)

        def end(a, zz, way):
            across(a, zz).wait_send()
            if way != 0:
                along(a, zz, z, zz).wait_send()

        order(end)
        if scount:
            exchange.finish()

    dma = pltpu.SemaphoreType.DMA
    return pl.pallas_call(
        body,
        out_shape=[jax.ShapeDtypeStruct((rows, width), F32)] * count
        + [jax.ShapeDtypeStruct((ndp, a.shape[0] // ndp, a.shape[1]), a.dtype) for a in shared],
        in_specs=[ANY] * (count + scount),
        out_specs=[pl.BlockSpec(memory_space=pltpu.VMEM)] * count + [ANY] * scount,
        scratch_shapes=[
            pltpu.VMEM((count, nz, rows, width), BF16),
            pltpu.VMEM((count, nz, rows, width), BF16),
            pltpu.VMEM((count, nz + 1, rows, width), BF16),
            dma((count, nz)),
            dma((count, nz)),
            dma((count, nz)),
            dma((count, nz)),
            dma((count, nz + 1)),
        ]
        + ([dma((scount, ndp)), dma((scount, ndp)), dma((scount,))] if scount else []),
        name=name,
        cost_estimate=takes(60 * count),
        compiler_params=pltpu.CompilerParams(has_side_effects=True, vmem_limit_bytes=VMEM_LIMIT),
    )(*parts, *shared)


def to_owners(name, n, ndp, blocks, owned):
    count = len(blocks)

    def body(*refs):
        ins, outs = refs[: count + 1], refs[count + 1 : 2 * count + 2]
        send, recv, local, one = refs[2 * count + 2 :]
        d, c = lax.axis_index("dp"), lax.axis_index("ctx")
        owner = c * ndp + d
        home = owner == d * n + c

        def give():
            return remote(ins[count], outs[count], one.at[0], one.at[1], (owner // n, lax.rem(owner, n)))

        def keep():
            return pltpu.make_async_copy(ins[count], outs[count], one.at[2])

        pl.when(home)(lambda: keep().start())
        pl.when(jnp.logical_not(home))(lambda: give().start())

        def rows_of(i, t):
            rows = blocks[i].shape[0] // n
            return ins[i].at[pl.ds(pl.multiple_of(t * rows, rows), rows), :]

        def columns_of(i, t):
            w = blocks[i].shape[1]
            return outs[i].at[:, pl.ds(pl.multiple_of(t * w, w), w)]

        def out(i, j):
            t = lax.rem(c + j, n)
            return remote(rows_of(i, t), columns_of(i, c), send.at[i, j], recv.at[i, c], (d, t))

        def back(i, j):
            t = lax.rem(c + j, n)
            return remote(rows_of(i, t), columns_of(i, t), send.at[i, j], recv.at[i, t], (d, t))

        def own(i):
            return pltpu.make_async_copy(rows_of(i, c), columns_of(i, c), local.at[i])

        for i in range(count):
            own(i).start()

        def go(j, carry):
            for i in range(count):
                out(i, j).start()
            return carry

        lax.fori_loop(1, n, go, 0)

        def done(j, carry):
            for i in range(count):
                out(i, j).wait_send()
                back(i, j).wait_recv()
            return carry

        lax.fori_loop(1, n, done, 0)
        for i in range(count):
            own(i).wait()
        pl.when(home)(lambda: keep().wait())
        pl.when(jnp.logical_not(home))(lambda: give().wait())

    dma = pltpu.SemaphoreType.DMA
    return pl.pallas_call(
        body,
        out_shape=[jax.ShapeDtypeStruct((b.shape[0] // n, b.shape[1] * n), b.dtype) for b in blocks]
        + [jax.ShapeDtypeStruct(owned.shape, owned.dtype)],
        in_specs=[ANY] * (count + 1),
        out_specs=[ANY] * (count + 1),
        scratch_shapes=[dma((count, n)), dma((count, n)), dma((count,)), dma((3,))],
        name=name,
        cost_estimate=takes(20),
        compiler_params=pltpu.CompilerParams(has_side_effects=True),
    )(*blocks, owned)


def swap_halves(x):
    width = x.shape[-1]
    lane = lax.broadcasted_iota(jnp.int32, x.shape, 1)
    half = HEAD_SIZE // 2
    up = pltpu.roll(x, width - half, 1)
    down = pltpu.roll(x, half, 1)
    return jnp.where(lane % HEAD_SIZE < half, up, down)


def attend_forward(query, key_value, cosine, sine, pos_rows, pos_cols, heads, block):
    length, width = query.shape
    kv_width = key_value.shape[1]
    scaling = 1.0 / math.sqrt(HEAD_SIZE)

    def body(q_ref, kv_ref, cos_ref, sin_ref, cosf_ref, sinf_ref, posq_ref, posk_ref, qr_ref, kvr_ref, o_ref, lse_ref):
        @pl.when(pl.program_id(0) == 0)
        def _():
            kv = kv_ref[:, : 2 * HEAD_SIZE]
            lane = lax.broadcasted_iota(jnp.int32, kv.shape, 1)
            rotated = kv * cosf_ref[:, : 2 * HEAD_SIZE] + swap_halves(kv) * sinf_ref[:, : 2 * HEAD_SIZE]
            kvr_ref[...] = jnp.where(lane < HEAD_SIZE, rotated, kv).astype(BF16)

        q = q_ref[...]
        q_rot = (q * cos_ref[...] + swap_halves(q) * sin_ref[...]).astype(BF16)
        qr_ref[...] = q_rot
        keys = kvr_ref[:, :HEAD_SIZE]
        values = kvr_ref[:, HEAD_SIZE : 2 * HEAD_SIZE]
        allowed = posk_ref[...] <= posq_ref[...]
        parts, stats = [], []
        for h in range(heads):
            q_head = q_rot[:, h * HEAD_SIZE : (h + 1) * HEAD_SIZE]
            s = lax.dot_general(q_head, keys, LAST_LAST, preferred_element_type=F32) * scaling
            s = jnp.where(allowed, s, NEG_FILL)
            top = jnp.max(s, axis=-1, keepdims=True)
            lse = top + jnp.log(jnp.sum(jnp.exp(s - top), axis=-1, keepdims=True))
            probs = jnp.exp(s - lse).astype(BF16)
            parts.append(jnp.dot(probs, values, preferred_element_type=F32).astype(BF16))
            stats.append(lse)
        if heads * HEAD_SIZE < width:
            parts.append(jnp.zeros((block, width - heads * HEAD_SIZE), BF16))
        o_ref[...] = jnp.concatenate(parts, axis=1)
        lse_ref[...] = jnp.concatenate(stats, axis=1)

    row = lambda i: (i, 0)
    whole = lambda i: (0, 0)
    return pl.pallas_call(
        body,
        grid=(length // block,),
        out_shape=[
            jax.ShapeDtypeStruct((length, width), BF16),
            jax.ShapeDtypeStruct((length, 2 * HEAD_SIZE), BF16),
            jax.ShapeDtypeStruct((length, width), BF16),
            jax.ShapeDtypeStruct((length, heads), F32),
        ],
        in_specs=[
            pl.BlockSpec((block, width), row),
            pl.BlockSpec((length, kv_width), whole),
            pl.BlockSpec((block, width), row),
            pl.BlockSpec((block, width), row),
            pl.BlockSpec((length, cosine.shape[1]), whole),
            pl.BlockSpec((length, cosine.shape[1]), whole),
            pl.BlockSpec((block, 1), row),
            pl.BlockSpec((1, length), whole),
        ],
        out_specs=[
            pl.BlockSpec((block, width), row),
            pl.BlockSpec((length, 2 * HEAD_SIZE), whole),
            pl.BlockSpec((block, width), row),
            pl.BlockSpec((block, heads), row),
        ],
        name="attend_forward",
        cost_estimate=takes(16),
        compiler_params=pltpu.CompilerParams(vmem_limit_bytes=VMEM_LIMIT),
    )(query, key_value, cosine[:, :width], sine[:, :width], cosine, sine, pos_rows, pos_cols)


def attend_backward(q_rot, kv_rot, attended, attended_gradient, lse, cosine, sine, pos_rows, pos_cols, heads, block):
    length, width = q_rot.shape
    scaling = 1.0 / math.sqrt(HEAD_SIZE)
    steps = length // block

    def body(q_ref, kv_ref, o_ref, do_ref, lse_ref, cos_ref, sin_ref, cosf_ref, sinf_ref, posq_ref, posk_ref, dq_ref, dkv_ref, dk_acc, dv_acc):
        @pl.when(pl.program_id(0) == 0)
        def _():
            dk_acc[...] = jnp.zeros_like(dk_acc)
            dv_acc[...] = jnp.zeros_like(dv_acc)

        keys = kv_ref[:, :HEAD_SIZE]
        values = kv_ref[:, HEAD_SIZE : 2 * HEAD_SIZE]
        allowed = posk_ref[...] <= posq_ref[...]
        parts = []
        for h in range(heads):
            at = slice(h * HEAD_SIZE, (h + 1) * HEAD_SIZE)
            q_head = q_ref[:, at]
            grad = do_ref[:, at]
            delta = jnp.sum(grad.astype(F32) * o_ref[:, at].astype(F32), axis=-1, keepdims=True)
            s = lax.dot_general(q_head, keys, LAST_LAST, preferred_element_type=F32) * scaling
            s = jnp.where(allowed, s, NEG_FILL)
            p = jnp.exp(s - lse_ref[:, h : h + 1])
            dp = lax.dot_general(grad, values, LAST_LAST, preferred_element_type=F32)
            ds = (p * (dp - delta)).astype(BF16)
            parts.append(jnp.dot(ds, keys, preferred_element_type=F32) * scaling)
            dk_acc[...] += lax.dot_general(ds, q_head, ROWS_FIRST, preferred_element_type=F32)
            dv_acc[...] += lax.dot_general(p.astype(BF16), grad, ROWS_FIRST, preferred_element_type=F32)
        if heads * HEAD_SIZE < width:
            parts.append(jnp.zeros((block, width - heads * HEAD_SIZE), F32))
        dq = jnp.concatenate(parts, axis=1)
        dq_ref[...] = (dq * cos_ref[...] - swap_halves(dq) * sin_ref[...]).astype(BF16)

        @pl.when(pl.program_id(0) == steps - 1)
        def _():
            dkv = jnp.concatenate([dk_acc[...] * scaling, dv_acc[...]], axis=1)
            lane = lax.broadcasted_iota(jnp.int32, dkv.shape, 1)
            rotated = dkv * cosf_ref[:, : 2 * HEAD_SIZE] - swap_halves(dkv) * sinf_ref[:, : 2 * HEAD_SIZE]
            dkv_ref[...] = jnp.where(lane < HEAD_SIZE, rotated, dkv).astype(BF16)

    row = lambda i: (i, 0)
    whole = lambda i: (0, 0)
    return pl.pallas_call(
        body,
        grid=(steps,),
        out_shape=[
            jax.ShapeDtypeStruct((length, width), BF16),
            jax.ShapeDtypeStruct((length, 2 * HEAD_SIZE), BF16),
        ],
        in_specs=[
            pl.BlockSpec((block, width), row),
            pl.BlockSpec((length, 2 * HEAD_SIZE), whole),
            pl.BlockSpec((block, width), row),
            pl.BlockSpec((block, width), row),
            pl.BlockSpec((block, heads), row),
            pl.BlockSpec((block, width), row),
            pl.BlockSpec((block, width), row),
            pl.BlockSpec((length, cosine.shape[1]), whole),
            pl.BlockSpec((length, cosine.shape[1]), whole),
            pl.BlockSpec((block, 1), row),
            pl.BlockSpec((1, length), whole),
        ],
        out_specs=[
            pl.BlockSpec((block, width), row),
            pl.BlockSpec((length, 2 * HEAD_SIZE), whole),
        ],
        scratch_shapes=[pltpu.VMEM((length, HEAD_SIZE), F32), pltpu.VMEM((length, HEAD_SIZE), F32)],
        name="attend_backward",
        cost_estimate=takes(20),
        compiler_params=pltpu.CompilerParams(vmem_limit_bytes=VMEM_LIMIT),
    )(q_rot, kv_rot, attended, attended_gradient, lse, cosine[:, :width], sine[:, :width], cosine, sine, pos_rows, pos_cols)


def gate_grads(grad_hidden, gate_pre, up_pre):
    sigmoid_gate = jax.nn.sigmoid(gate_pre)
    swish_gate = gate_pre * sigmoid_gate
    grad_gate_pre = (
        grad_hidden * up_pre * sigmoid_gate * (1.0 + gate_pre * (1.0 - sigmoid_gate))
    ).astype(BF16)
    return (grad_gate_pre, (grad_hidden * swish_gate).astype(BF16))


def on_device(
    ndp,
    n,
    block_input,
    piece_order,
    attention_gain,
    query_weight,
    key_matrix,
    value_matrix,
    output_weight,
    feed_gain,
    gate_weight,
    up_weight,
    down_weight,
    cotangent,
):
    _, t, width = block_input.shape
    length = n * t
    rows = query_weight.shape[0]
    heads = QUERY_HEADS // n
    q_width = heads * HEAD_SIZE
    copies = max(1, n // KEY_VALUE_HEADS)
    piece_rows = t // 2

    x_rows = block_input[0]
    grad_rows = cotangent[0]

    offsets = jnp.arange(piece_rows, dtype=jnp.int32)
    pos = ((piece_order * piece_rows)[:, :, None] + offsets[None, None, :]).reshape(-1)
    half = HEAD_SIZE // 2
    frequency = jnp.exp(jnp.arange(half, dtype=F32) * (-2.0 * math.log(ROPE_BASE) / HEAD_SIZE))
    angle = pos.astype(F32)[:, None] * frequency[None, :]
    cos_half, sin_half = jnp.cos(angle), jnp.sin(angle)
    table_heads = max(heads, 2)
    cosine = jnp.tile(jnp.concatenate([cos_half, cos_half], axis=1), (1, table_heads))
    sine = jnp.tile(jnp.concatenate([-sin_half, sin_half], axis=1), (1, table_heads))
    pos_rows, pos_cols = pos[:, None], pos[None, :]
    block = min(256, length)

    def per_head(matrix):
        return jnp.repeat(matrix.reshape(rows, KEY_VALUE_HEADS, HEAD_SIZE), copies, axis=1)

    gains = jnp.stack([attention_gain, feed_gain], axis=1)
    gains = jnp.broadcast_to(jnp.pad(gains, ((0, 0), (0, 126)))[:, None, :], (rows, n, 128))
    kv_gain = jnp.concatenate([per_head(key_matrix), per_head(value_matrix), gains], axis=2)
    kv_gain = kv_gain.reshape(rows, n * 256)
    down_rows = down_weight.T
    q_columns = max(q_width, 128)
    query_columns = query_weight
    if q_columns > q_width:
        query_columns = jnp.pad(
            query_weight.reshape(rows, n, q_width), ((0, 0), (0, 0), (0, q_columns - q_width))
        ).reshape(rows, n * q_columns)

    x_all, w_query, w_kv, w_output = fetch(
        "fetch_first", n, ndp, [x_rows], [query_columns, kv_gain], output_weight
    )
    w_output = w_output.reshape(q_width, width)
    x_all, gate_weight, up_weight, down_rows, grad_rows = lax.optimization_barrier(
        (x_all, gate_weight, up_weight, down_rows, grad_rows)
    )
    grad_all = lax.all_gather(grad_rows, "ctx", axis=0, tiled=True)
    gate_cols, up_cols, down_cols = (
        lax.all_gather(pass_blocks(w, n, 1, 0), "dp", axis=0, tiled=True)
        for w in (gate_weight, up_weight, down_rows)
    )
    gain_attention = w_kv[:, 128].astype(F32)
    gain_feed = w_kv[:, 129].astype(F32)

    x_all = x_all.reshape(length, width)
    unit_all, _ = normalize(x_all.astype(F32))
    normed_one = (unit_all * gain_attention).astype(BF16)
    query = jnp.dot(normed_one, w_query, preferred_element_type=F32)
    key_value = jnp.dot(normed_one, w_kv, preferred_element_type=F32)
    q_rot, kv_rot, attended, lse = attend_forward(
        query, key_value, cosine, sine, pos_rows, pos_cols, heads, block
    )
    attended = attended[:, :q_width]
    part = jnp.dot(attended, w_output, preferred_element_type=F32).astype(BF16)
    (attended_sum,) = scatter_sum("attended_sum", n, [part.reshape(n, t, width)])
    inputs32 = x_rows.astype(F32)
    unit_one, inv_one = normalize(inputs32)
    mid = inputs32 + attended_sum
    unit_two, inv_two = normalize(mid)
    normed_rows = (unit_two * gain_feed).astype(BF16)
    (normed_all,) = fetch("gather_normed", n, ndp, [normed_rows], [])
    normed_all = normed_all.reshape(length, width)

    gate_pre = jnp.dot(normed_all, gate_cols, preferred_element_type=F32)
    up_pre = jnp.dot(normed_all, up_cols, preferred_element_type=F32)
    hidden = (jax.nn.silu(gate_pre) * up_pre).astype(BF16)
    grad_hidden = jnp.dot(grad_all, down_cols, preferred_element_type=F32)
    grad_gate_pre, grad_up_pre = gate_grads(grad_hidden, gate_pre, up_pre)
    block_part = lax.dot_general(hidden, down_cols, LAST_LAST, preferred_element_type=F32).astype(BF16)
    normed_part = (
        lax.dot_general(grad_gate_pre, gate_cols, LAST_LAST, preferred_element_type=F32)
        + lax.dot_general(grad_up_pre, up_cols, LAST_LAST, preferred_element_type=F32)
    ).astype(BF16)
    term_gate = lax.dot_general(normed_all, grad_gate_pre, ROWS_FIRST, preferred_element_type=F32)
    term_up = lax.dot_general(normed_all, grad_up_pre, ROWS_FIRST, preferred_element_type=F32)
    term_down = lax.dot_general(grad_all, hidden, ROWS_FIRST, preferred_element_type=F32)
    terms = tuple(term.astype(BF16) for term in (term_gate, term_up, term_down))
    normed_part, block_part, terms = lax.optimization_barrier((normed_part, block_part, terms))
    gate_sum, up_sum, down_sum = (
        lax.psum_scatter(term, "dp", scatter_dimension=0, tiled=True) for term in terms
    )
    grad_normed_two, block_sum = scatter_sum(
        "feed_sum", n, [normed_part.reshape(n, t, width), block_part.reshape(n, t, width)]
    )
    block_output = (mid + block_sum).astype(BF16)[None]
    grad_unit_two = grad_normed_two * gain_feed
    grad_mid = grad_rows.astype(F32) + inv_two * (
        grad_unit_two - unit_two * jnp.mean(grad_unit_two * unit_two, axis=-1, keepdims=True)
    )

    (grad_mid_all,) = fetch("gather_mid", n, ndp, [grad_mid.astype(BF16)], [])
    grad_mid_all = grad_mid_all.reshape(length, width)
    attended_gradient = lax.dot_general(
        grad_mid_all, w_output, LAST_LAST, preferred_element_type=F32
    ).astype(BF16)
    term_output = lax.dot_general(attended, grad_mid_all, ROWS_FIRST, preferred_element_type=F32)
    fill = ((0, 0), (0, q_columns - q_width))
    grad_query, grad_kv = attend_backward(
        q_rot, kv_rot, jnp.pad(attended, fill), jnp.pad(attended_gradient, fill), lse, cosine, sine, pos_rows, pos_cols, heads, block
    )
    one_part = (
        lax.dot_general(grad_query, w_query, LAST_LAST, preferred_element_type=F32)
        + lax.dot_general(grad_kv, w_kv[:, :128], LAST_LAST, preferred_element_type=F32)
    ).astype(BF16)
    term_query = lax.dot_general(normed_one, grad_query, ROWS_FIRST, preferred_element_type=F32)
    term_kv = lax.dot_general(normed_one, grad_kv, ROWS_FIRST, preferred_element_type=F32)
    own_gate, own_up, own_down = (pass_blocks(term, n, 0, 1) for term in (gate_sum, up_sum, down_sum))
    grad_normed_one, query_terms, kv_terms, output_terms = scatter_sum(
        "one_sum",
        n,
        [one_part.reshape(n, t, width)],
        ndp,
        [term_query.astype(BF16), term_kv.astype(BF16), term_output.astype(BF16)],
    )
    query_sum, kv_sum, output_sum = (
        jnp.sum(terms.astype(F32), axis=0).astype(BF16) for terms in (query_terms, kv_terms, output_terms)
    )
    own_query, own_kv, own_output = to_owners("to_owners", n, ndp, [query_sum, kv_sum], output_sum)
    grad_output_w = own_output.astype(F32)
    grad_gate_w, grad_up_w = own_gate.astype(F32), own_up.astype(F32)
    grad_down_w = own_down.astype(F32).T
    grad_query_w = own_query.astype(F32)
    if q_columns > q_width:
        grad_query_w = grad_query_w.reshape(rows, n, q_columns)[:, :, :q_width].reshape(rows, n * q_width)
    own_kv = own_kv.astype(F32).reshape(rows, KEY_VALUE_HEADS, copies, 2, HEAD_SIZE).sum(axis=2)
    grad_key_w = own_kv[:, :, 0].reshape(rows, KEY_VALUE_HEADS * HEAD_SIZE)
    grad_value_w = own_kv[:, :, 1].reshape(rows, KEY_VALUE_HEADS * HEAD_SIZE)

    def product(grad, weight):
        return jnp.sum(grad * weight.astype(F32), axis=1)

    grad_attention_w = (
        product(grad_query_w, query_weight)
        + product(grad_key_w, key_matrix)
        + product(grad_value_w, value_matrix)
    ) / attention_gain.astype(F32)
    grad_feed_w = (product(grad_gate_w, gate_weight) + product(grad_up_w, up_weight)) / feed_gain.astype(F32)

    grad_unit_one = grad_normed_one * gain_attention
    input_grad = grad_mid + inv_one * (
        grad_unit_one - unit_one * jnp.mean(grad_unit_one * unit_one, axis=-1, keepdims=True)
    )
    return (
        block_output,
        input_grad.astype(BF16)[None],
        grad_attention_w,
        grad_query_w,
        grad_key_w,
        grad_value_w,
        grad_output_w,
        grad_feed_w,
        grad_gate_w,
        grad_up_w,
        grad_down_w,
    )


def solution(mesh):
    return jax.shard_map(
        functools.partial(on_device, mesh.shape["dp"], mesh.shape["ctx"]),
        mesh=mesh,
        in_specs=(
            P("dp", "ctx", None),
            P(),
            P(("dp", "ctx")),
            P(("dp", "ctx"), None),
            P(("dp", "ctx"), None),
            P(("dp", "ctx"), None),
            P(("dp", "ctx"), None),
            P(("dp", "ctx")),
            P(("dp", "ctx"), None),
            P(("dp", "ctx"), None),
            P(None, ("dp", "ctx")),
            P("dp", "ctx", None),
        ),
        out_specs=(
            P("dp", "ctx", None),
            P("dp", "ctx", None),
            P(("dp", "ctx")),
            P(("dp", "ctx"), None),
            P(("dp", "ctx"), None),
            P(("dp", "ctx"), None),
            P(("dp", "ctx"), None),
            P(("dp", "ctx")),
            P(("dp", "ctx"), None),
            P(("dp", "ctx"), None),
            P(None, ("dp", "ctx")),
        ),
        check_vma=False,
    )
```

```python
import functools
import math

import jax
import jax.numpy as jnp
from jax import lax
from jax.experimental import pallas as pl
from jax.experimental.pallas import tpu as pltpu
from jax.sharding import PartitionSpec as P

QUERY_HEADS = 32
KEY_VALUE_HEADS = 8
HEAD_SIZE = 64
EPSILON = 1e-05
ROPE_BASE = 500000.0
NEG_FILL = -1e30
ROWS_FIRST = (((0,), (0,)), ((), ()))
LAST_LAST = (((1,), (1,)), ((), ()))
MESH = pl.DeviceIdType.MESH
F32 = jnp.float32
BF16 = jnp.bfloat16
ANY = pl.BlockSpec(memory_space=pl.ANY)
VMEM_LIMIT = 60 * 1024 * 1024


def normalize(rows_in):
    inv_rms = lax.rsqrt(jnp.mean(rows_in * rows_in, axis=-1, keepdims=True) + EPSILON)
    return (rows_in * inv_rms, inv_rms)


def takes(us):
    return pl.CostEstimate(flops=0, bytes_accessed=int(us * 3.5e6), transcendentals=0)


def remote(src, dst, send, recv, dev):
    return pltpu.make_async_remote_copy(
        src_ref=src, dst_ref=dst, send_sem=send, recv_sem=recv, device_id=dev, device_id_type=MESH
    )


DMA = pltpu.SemaphoreType.DMA
IN_VMEM = pl.BlockSpec(memory_space=pltpu.VMEM)


def block_rows(ref, rows, t):
    return ref.at[pl.ds(pl.multiple_of(t * rows, rows), rows), :]


def block_columns(ref, width, t):
    return ref.at[:, pl.ds(pl.multiple_of(t * width, width), width)]


def either(condition, yes, no):
    pl.when(condition)(yes)
    pl.when(jnp.logical_not(condition))(no)


class Work:
    arrays, outs, scratch = (), (), ()

    def place(self):
        self.d, self.c = lax.axis_index("dp"), lax.axis_index("ctx")

    def steps(self, early, late):
        early()
        late()

    def early(self):
        pass

    def late(self):
        pass


class Gather(Work):
    main = True

    def __init__(self, n, rows):
        self.n, self.nz, self.arrays = n, n // 2, [rows]
        self.outs = [(jax.ShapeDtypeStruct((n,) + rows.shape, rows.dtype), ANY)]
        self.scratch = [DMA((2, n // 2)), DMA((n,)), DMA((n,)), DMA((1,))]

    def bind(self, ins, outs, scratch):
        self.place()
        (self.src,), (self.dst,) = ins, outs
        self.send, self.send_pair, self.recv, self.local = scratch
        self.z, self.y = self.c // 2, lax.rem(self.c, 2)

    def first(self, tz, ty, sem):
        return remote(self.src, self.dst.at[self.c], sem, self.recv.at[self.c], (self.d, tz * 2 + ty))

    def onward(self, s, tz, ty, sem):
        return remote(self.dst.at[s], self.dst.at[s], sem, self.recv.at[s], (self.d, tz * 2 + ty))

    def own(self):
        return pltpu.make_async_copy(self.src, self.dst.at[self.c], self.local.at[0])

    def start(self):
        z, y, nz = self.z, self.y, self.nz
        pl.when(z + 1 < nz)(lambda: self.first(z + 1, y, self.send.at[0, 0]).start())
        pl.when(z > 0)(lambda: self.first(z - 1, y, self.send.at[1, 0]).start())
        self.first(z, 1 - y, self.send_pair.at[0]).start()
        self.own().start()

    def steps(self, early, late):
        z, y, nz = self.z, self.y, self.nz
        for k in range(1, nz):

            @pl.when(z - k >= 0)
            def _():
                s = (z - k) * 2 + y
                self.onward(s, z, y, self.send.at[0, k]).wait_recv()
                pl.when(z + 1 < nz)(lambda: self.onward(s, z + 1, y, self.send.at[0, k]).start())
                self.onward(s, z, 1 - y, self.send_pair.at[k]).start()

            @pl.when(z + k < nz)
            def _():
                s = (z + k) * 2 + y
                self.onward(s, z, y, self.send.at[1, k]).wait_recv()
                pl.when(z > 0)(lambda: self.onward(s, z - 1, y, self.send.at[1, k]).start())
                self.onward(s, z, 1 - y, self.send_pair.at[nz - 1 + k]).start()

            if k == 1:
                early()
        late()

    def finish(self):
        z, y, nz = self.z, self.y, self.nz
        self.own().wait()

        def arrived(zz, carry):
            self.onward(zz * 2 + 1 - y, z, y, self.send.at[0, 0]).wait_recv()
            return carry

        lax.fori_loop(0, nz, arrived, 0)
        self.first(z, 1 - y, self.send_pair.at[0]).wait_send()
        pl.when(z + 1 < nz)(lambda: self.first(z + 1, y, self.send.at[0, 0]).wait_send())
        pl.when(z > 0)(lambda: self.first(z - 1, y, self.send.at[1, 0]).wait_send())
        for k in range(1, nz):

            @pl.when(z - k >= 0)
            def _():
                s = (z - k) * 2 + y
                pl.when(z + 1 < nz)(lambda: self.onward(s, z + 1, y, self.send.at[0, k]).wait_send())
                self.onward(s, z, 1 - y, self.send_pair.at[k]).wait_send()

            @pl.when(z + k < nz)
            def _():
                s = (z + k) * 2 + y
                pl.when(z > 0)(lambda: self.onward(s, z - 1, y, self.send.at[1, k]).wait_send())
                self.onward(s, z, 1 - y, self.send_pair.at[nz - 1 + k]).wait_send()


class RowSum(Work):
    main = True

    def __init__(self, n, part):
        self.n, self.nz, self.arrays = n, n // 2, [part]
        _, self.rows, width = part.shape
        nz, shape = self.nz, (self.rows, width)
        self.outs = [(jax.ShapeDtypeStruct(shape, F32), IN_VMEM)]
        self.scratch = [
            pltpu.VMEM((nz,) + shape, BF16),
            pltpu.VMEM((nz,) + shape, BF16),
            pltpu.VMEM((nz + 1,) + shape, BF16),
            DMA((nz,)),
            DMA((nz,)),
            DMA((nz,)),
            DMA((nz,)),
            DMA((nz + 1,)),
        ]

    def bind(self, ins, outs, scratch):
        self.place()
        (self.src,), (self.out,) = ins, outs
        self.own, self.pair, self.far, self.s_own, self.s_pair, self.r_pair, self.s_far, self.r_far = scratch
        self.z, self.y = self.c // 2, lax.rem(self.c, 2)

    def load(self, zz):
        return pltpu.make_async_copy(self.src.at[zz * 2 + self.y], self.own.at[zz], self.s_own.at[zz])

    def across(self, zz):
        dev = (self.d, self.z * 2 + 1 - self.y)
        return remote(
            self.src.at[zz * 2 + 1 - self.y], self.pair.at[zz], self.s_pair.at[zz], self.r_pair.at[zz], dev
        )

    def along(self, zz, tz, slot):
        dev = (self.d, tz * 2 + self.y)
        return remote(self.pair.at[zz], self.far.at[slot], self.s_far.at[zz], self.r_far.at[slot], dev)

    def order(self, fn, between=None):
        z, nz = self.z, self.nz
        for k in range(nz - 1, 0, -1):
            pl.when(z - k >= 0)(functools.partial(fn, z - k, -1))
            pl.when(z + k < nz)(functools.partial(fn, z + k, 1))
        if between is not None:
            between()
        fn(z, 0)

    def begin(self, zz, way):
        self.across(zz).start()
        self.load(zz).start()

    def add(self, zz, slots, out):
        step = 32

        def chunk(i, carry):
            at = pl.ds(pl.multiple_of(i * step, step), step)
            total = self.own[zz, at, :].astype(F32) + self.pair[zz, at, :].astype(F32)
            for slot in slots:
                total = total + self.far[slot, at, :].astype(F32)
            if out is None:
                self.pair[zz, at, :] = total.astype(BF16)
            else:
                out[at, :] = total
            return carry

        lax.fori_loop(0, self.rows // step, chunk, 0)

    def handle(self, zz, way):
        z, nz = self.z, self.nz
        self.load(zz).wait()
        self.across(zz).wait_recv()
        if way == 0:
            pl.when(z > 0)(lambda: self.along(z, z, z).wait_recv())
            pl.when(z + 1 < nz)(lambda: self.along(z, z, nz).wait_recv())
            pl.when(z == 0)(lambda: self.add(z, (nz,), self.out))
            pl.when(z + 1 == nz)(lambda: self.add(z, (z,), self.out))
            pl.when((z > 0) & (z + 1 < nz))(lambda: self.add(z, (z, nz), self.out))
            return
        behind = z - way

        def with_behind():
            self.along(zz, z, zz).wait_recv()
            self.add(zz, (zz,), None)

        either((behind >= 0) & (behind < nz), with_behind, lambda: self.add(zz, (), None))
        tz = z + way
        if way < 0:
            either(
                tz == zz,
                lambda: self.along(zz, tz, nz).start(),
                lambda: self.along(zz, tz, zz).start(),
            )
        else:
            self.along(zz, tz, zz).start()

    def end(self, zz, way):
        self.across(zz).wait_send()
        if way != 0:
            self.along(zz, self.z, zz).wait_send()

    def start(self):
        self.order(self.begin)

    def steps(self, early, late):
        early()
        self.order(self.handle, late)

    def finish(self):
        self.order(self.end)


class WeightFetch(Work):
    def __init__(self, n, ndp, array):
        self.n, self.arrays = n, [array]
        self.rows, self.width = array.shape[0], array.shape[1] // n
        total = n * ndp
        self.outs = [(jax.ShapeDtypeStruct((self.rows * total, self.width), array.dtype), ANY)]
        self.scratch = [DMA((n,)), DMA((n,)), DMA((2 * n,)), DMA((total,)), DMA((1,))]

    def bind(self, ins, outs, scratch):
        self.place()
        (self.src,), (self.dst,) = ins, outs
        self.out_sem, self.x_sem, self.core_sem, self.recv, self.local = scratch
        self.d_core = self.d + 1 - 2 * lax.rem(self.d, 2)
        self.d_x = lax.rem(self.d + 2, 4)
        self.me = self.d * self.n + self.c

    def block(self, r):
        return block_rows(self.dst, self.rows, r)

    def spread(self, j):
        t = lax.rem(self.c + j, self.n)
        part = block_columns(self.src, self.width, t)
        return remote(part, self.block(self.me), self.out_sem.at[j], self.recv.at[self.me], (self.d, t))

    def own_to(self, dev_d, sem):
        part = block_columns(self.src, self.width, self.c)
        return remote(part, self.block(self.me), sem, self.recv.at[self.me], (dev_d, self.c))

    def pass_on(self, r, dev_d, sem):
        return remote(self.block(r), self.block(r), sem, self.recv.at[r], (dev_d, self.c))

    def own(self):
        part = block_columns(self.src, self.width, self.c)
        return pltpu.make_async_copy(part, self.block(self.me), self.local.at[0])

    def start(self):
        self.own_to(self.d_x, self.x_sem.at[0]).start()
        self.own_to(self.d_core, self.core_sem.at[0]).start()
        self.own().start()

        def go(j, carry):
            self.spread(j).start()
            return carry

        lax.fori_loop(1, self.n, go, 0)

    def early(self):
        n = self.n

        def same(j, carry):
            r = self.d * n + lax.rem(self.c + n - j, n)
            self.pass_on(r, self.d_x, self.x_sem.at[j]).wait_recv()
            self.pass_on(r, self.d_x, self.x_sem.at[j]).start()
            self.pass_on(r, self.d_core, self.core_sem.at[j]).start()
            return carry

        lax.fori_loop(1, n, same, 0)

    def late(self):
        n = self.n

        def across(j, carry):
            r = self.d_x * n + lax.rem(self.c + n - j, n)
            self.pass_on(r, self.d_core, self.core_sem.at[n + j]).wait_recv()
            self.pass_on(r, self.d_core, self.core_sem.at[n + j]).start()
            return carry

        lax.fori_loop(0, n, across, 0)

    def finish(self):
        n = self.n
        d_far = lax.rem(self.d_core + 2, 4)
        self.own().wait()
        self.own_to(self.d_x, self.x_sem.at[0]).wait_send()
        self.own_to(self.d_core, self.core_sem.at[0]).wait_send()

        def last(j, carry):
            cc = lax.rem(self.c + n - j, n)
            self.pass_on(self.d_core * n + cc, self.d_core, self.core_sem.at[0]).wait_recv()
            self.pass_on(d_far * n + cc, self.d_core, self.core_sem.at[0]).wait_recv()
            self.pass_on(self.d_x * n + cc, self.d_core, self.core_sem.at[n + j]).wait_send()
            return carry

        lax.fori_loop(0, n, last, 0)

        def sent(j, carry):
            r = self.d * n + lax.rem(self.c + n - j, n)
            self.spread(j).wait_send()
            self.pass_on(r, self.d_x, self.x_sem.at[j]).wait_send()
            self.pass_on(r, self.d_core, self.core_sem.at[j]).wait_send()
            return carry

        lax.fori_loop(1, n, sent, 0)


class OwnerSpread(Work):
    def __init__(self, n, ndp, array):
        self.n, self.ndp, self.arrays = n, ndp, [array]
        self.outs = [(jax.ShapeDtypeStruct((ndp,) + array.shape, array.dtype), ANY)]
        self.scratch = [DMA((ndp,)), DMA((ndp,)), DMA((1,))]

    def bind(self, ins, outs, scratch):
        self.place()
        (self.src,), (self.dst,) = ins, outs
        self.send, self.recv, self.local = scratch
        me = self.d * self.n + self.c
        self.target, self.slot = me // self.ndp, lax.rem(me, self.ndp)
        self.mine = (self.slot == self.d) & (self.target == self.c)
        self.away = jnp.logical_not(self.mine)

    def first(self):
        dev = (self.slot, self.target)
        return remote(self.src, self.dst.at[self.slot], self.send.at[0], self.recv.at[self.slot], dev)

    def own(self):
        return pltpu.make_async_copy(self.src, self.dst.at[self.d], self.local.at[0])

    def onward(self, k):
        t = lax.rem(self.d + k, self.ndp)
        return remote(self.dst.at[self.d], self.dst.at[self.d], self.send.at[k], self.recv.at[self.d], (t, self.c))

    def back(self, k):
        t = lax.rem(self.d + k, self.ndp)
        return remote(self.dst.at[t], self.dst.at[t], self.send.at[k], self.recv.at[t], (t, self.c))

    def start(self):
        either(self.mine, lambda: self.own().start(), lambda: self.first().start())

    def late(self):
        either(self.mine, lambda: self.own().wait(), lambda: self.onward(1).wait_recv())
        for k in range(1, self.ndp):
            self.onward(k).start()

    def finish(self):
        pl.when(self.away)(lambda: self.first().wait_send())
        for k in range(1, self.ndp):
            self.onward(k).wait_send()
            self.back(k).wait_recv()


class AllToAll(Work):
    def __init__(self, n, array, to_rows):
        self.n, self.to_rows, self.arrays = n, to_rows, [array]
        rows, width = array.shape
        if to_rows:
            self.rows, self.width = rows, width // n
            shape = (rows * n, width // n)
        else:
            self.rows, self.width = rows // n, width
            shape = (rows // n, width * n)
        self.outs = [(jax.ShapeDtypeStruct(shape, array.dtype), ANY)]
        self.scratch = [DMA((n,)), DMA((n,)), DMA((1,))]

    def bind(self, ins, outs, scratch):
        self.place()
        (self.src,), (self.dst,) = ins, outs
        self.send, self.recv, self.local = scratch

    def columns(self, ref, t):
        return block_columns(ref, self.width, t)

    def rows_of(self, ref, t):
        return block_rows(ref, self.rows, t)

    def part(self, t):
        return self.columns(self.src, t) if self.to_rows else self.rows_of(self.src, t)

    def home(self, t):
        return self.rows_of(self.dst, t) if self.to_rows else self.columns(self.dst, t)

    def out(self, j):
        t = lax.rem(self.c + j, self.n)
        return remote(self.part(t), self.home(self.c), self.send.at[j], self.recv.at[self.c], (self.d, t))

    def back(self, j):
        t = lax.rem(self.c + j, self.n)
        return remote(self.part(t), self.home(t), self.send.at[j], self.recv.at[t], (self.d, t))

    def own(self):
        return pltpu.make_async_copy(self.part(self.c), self.home(self.c), self.local.at[0])

    def start(self):
        def go(j, carry):
            self.out(j).start()
            return carry

        lax.fori_loop(1, self.n, go, 0)
        self.own().start()

    def finish(self):
        def done(j, carry):
            self.out(j).wait_send()
            self.back(j).wait_recv()
            return carry

        lax.fori_loop(1, self.n, done, 0)
        self.own().wait()


class DpSum(Work):
    def __init__(self, ndp, array):
        self.ndp, self.arrays = ndp, [array]
        self.size, width = array.shape[0] // ndp, array.shape[1]
        self.block_shape = (self.size, width)
        self.outs = [(jax.ShapeDtypeStruct(self.block_shape, BF16), IN_VMEM)]
        self.scratch = [pltpu.VMEM((ndp,) + self.block_shape, BF16), DMA((ndp,)), DMA((ndp,)), DMA((1,))]

    def bind(self, ins, outs, scratch):
        self.place()
        (self.src,), (self.total,) = ins, outs
        self.held, self.send, self.recv, self.local = scratch

    def copy(self, k):
        t = lax.rem(self.d + k, self.ndp)
        part = block_rows(self.src, self.size, t)
        return remote(part, self.held.at[self.d], self.send.at[k], self.recv.at[self.d], (t, self.c))

    def back(self, k):
        t = lax.rem(self.d + k, self.ndp)
        part = block_rows(self.src, self.size, t)
        return remote(part, self.held.at[t], self.send.at[k], self.recv.at[t], (t, self.c))

    def own(self):
        return pltpu.make_async_copy(block_rows(self.src, self.size, self.d), self.held.at[self.d], self.local.at[0])

    def start(self):
        for k in range(1, self.ndp):
            self.copy(k).start()
        self.own().start()

    def late(self):
        for k in range(1, self.ndp):
            self.copy(k).wait_send()
            self.back(k).wait_recv()
        self.own().wait()
        step = min(self.size, 32)

        def chunk(i, carry):
            at = pl.ds(pl.multiple_of(i * step, step), step)
            value = self.held[0, at, :].astype(F32)
            for j in range(1, self.ndp):
                value = value + self.held[j, at, :].astype(F32)
            self.total[at, :] = value.astype(BF16)
            return carry

        lax.fori_loop(0, self.size // step, chunk, 0)

    def finish(self):
        pass


class SumToColumns(DpSum):
    def __init__(self, n, ndp, array):
        super().__init__(ndp, array)
        self.move = AllToAll(n, self.outs[0][0], False)
        self.outs = self.move.outs
        self.scratch = self.scratch + [pltpu.VMEM(self.block_shape, BF16)] + self.move.scratch

    def bind(self, ins, outs, scratch):
        super().bind(ins, [scratch[4]], scratch[:4])
        self.move.bind([scratch[4]], outs, scratch[5:])

    def late(self):
        super().late()
        self.move.start()

    def finish(self):
        self.move.finish()


class SumToOwner(DpSum):
    def __init__(self, n, ndp, array):
        super().__init__(ndp, array)
        self.n = n
        self.outs = [(self.outs[0][0], ANY)]
        self.scratch = self.scratch + [pltpu.VMEM(self.block_shape, BF16), DMA((3,))]

    def bind(self, ins, outs, scratch):
        super().bind(ins, [scratch[4]], scratch[:4])
        (self.out,), self.one = outs, scratch[5]
        self.owner = self.c * self.ndp + self.d
        self.home = self.owner == self.d * self.n + self.c

    def give(self):
        dev = (self.owner // self.n, lax.rem(self.owner, self.n))
        return remote(self.total, self.out, self.one.at[0], self.one.at[1], dev)

    def keep(self):
        return pltpu.make_async_copy(self.total, self.out, self.one.at[2])

    def late(self):
        super().late()
        either(self.home, lambda: self.keep().start(), lambda: self.give().start())

    def finish(self):
        either(self.home, lambda: self.keep().wait(), lambda: self.give().wait())


def transfer(name, *works):
    arrays = [a for w in works for a in w.arrays]
    outs = [o for w in works for o in w.outs]
    scratch = [x for w in works for x in w.scratch]

    def body(*refs):
        refs = list(refs)
        ins, refs = refs[: len(arrays)], refs[len(arrays) :]
        results, refs = refs[: len(outs)], refs[len(outs) :]
        for w in works:
            w.bind(ins[: len(w.arrays)], results[: len(w.outs)], refs[: len(w.scratch)])
            ins, results, refs = ins[len(w.arrays) :], results[len(w.outs) :], refs[len(w.scratch) :]
        for w in works:
            w.start()

        def early():
            for w in works[1:]:
                w.early()

        def late():
            for w in works[1:]:
                w.late()

        works[0].steps(early, late)
        for w in works:
            w.finish()

    return pl.pallas_call(
        body,
        out_shape=[o[0] for o in outs],
        in_specs=[ANY] * len(arrays),
        out_specs=[o[1] for o in outs],
        scratch_shapes=scratch,
        name=name,
        cost_estimate=takes(60),
        compiler_params=pltpu.CompilerParams(has_side_effects=True, vmem_limit_bytes=VMEM_LIMIT),
    )(*arrays)


def swap_halves(x):
    width = x.shape[-1]
    lane = lax.broadcasted_iota(jnp.int32, x.shape, 1)
    half = HEAD_SIZE // 2
    up = pltpu.roll(x, width - half, 1)
    down = pltpu.roll(x, half, 1)
    return jnp.where(lane % HEAD_SIZE < half, up, down)


def attend_forward(query, key_value, cosine, sine, pos_rows, pos_cols, heads, block):
    length, width = query.shape
    kv_width = key_value.shape[1]
    scaling = 1.0 / math.sqrt(HEAD_SIZE)

    def body(q_ref, kv_ref, cos_ref, sin_ref, cosf_ref, sinf_ref, posq_ref, posk_ref, qr_ref, kvr_ref, o_ref, lse_ref):
        @pl.when(pl.program_id(0) == 0)
        def _():
            kv = kv_ref[:, : 2 * HEAD_SIZE]
            lane = lax.broadcasted_iota(jnp.int32, kv.shape, 1)
            rotated = kv * cosf_ref[:, : 2 * HEAD_SIZE] + swap_halves(kv) * sinf_ref[:, : 2 * HEAD_SIZE]
            kvr_ref[...] = jnp.where(lane < HEAD_SIZE, rotated, kv).astype(BF16)

        q = q_ref[...]
        q_rot = (q * cos_ref[...] + swap_halves(q) * sin_ref[...]).astype(BF16)
        qr_ref[...] = q_rot
        keys = kvr_ref[:, :HEAD_SIZE]
        values = kvr_ref[:, HEAD_SIZE : 2 * HEAD_SIZE]
        allowed = posk_ref[...] <= posq_ref[...]
        parts, stats = [], []
        for h in range(heads):
            q_head = q_rot[:, h * HEAD_SIZE : (h + 1) * HEAD_SIZE]
            s = lax.dot_general(q_head, keys, LAST_LAST, preferred_element_type=F32) * scaling
            s = jnp.where(allowed, s, NEG_FILL)
            top = jnp.max(s, axis=-1, keepdims=True)
            lse = top + jnp.log(jnp.sum(jnp.exp(s - top), axis=-1, keepdims=True))
            probs = jnp.exp(s - lse).astype(BF16)
            parts.append(jnp.dot(probs, values, preferred_element_type=F32).astype(BF16))
            stats.append(lse)
        if heads * HEAD_SIZE < width:
            parts.append(jnp.zeros((block, width - heads * HEAD_SIZE), BF16))
        o_ref[...] = jnp.concatenate(parts, axis=1)
        lse_ref[...] = jnp.concatenate(stats, axis=1)

    row = lambda i: (i, 0)
    whole = lambda i: (0, 0)
    return pl.pallas_call(
        body,
        grid=(length // block,),
        out_shape=[
            jax.ShapeDtypeStruct((length, width), BF16),
            jax.ShapeDtypeStruct((length, 2 * HEAD_SIZE), BF16),
            jax.ShapeDtypeStruct((length, width), BF16),
            jax.ShapeDtypeStruct((length, heads), F32),
        ],
        in_specs=[
            pl.BlockSpec((block, width), row),
            pl.BlockSpec((length, kv_width), whole),
            pl.BlockSpec((block, width), row),
            pl.BlockSpec((block, width), row),
            pl.BlockSpec((length, cosine.shape[1]), whole),
            pl.BlockSpec((length, cosine.shape[1]), whole),
            pl.BlockSpec((block, 1), row),
            pl.BlockSpec((1, length), whole),
        ],
        out_specs=[
            pl.BlockSpec((block, width), row),
            pl.BlockSpec((length, 2 * HEAD_SIZE), whole),
            pl.BlockSpec((block, width), row),
            pl.BlockSpec((block, heads), row),
        ],
        name="attend_forward",
        cost_estimate=takes(16),
        compiler_params=pltpu.CompilerParams(vmem_limit_bytes=VMEM_LIMIT),
    )(query, key_value, cosine[:, :width], sine[:, :width], cosine, sine, pos_rows, pos_cols)


def attend_backward(q_rot, kv_rot, attended, attended_gradient, lse, cosine, sine, pos_rows, pos_cols, heads, block):
    length, width = q_rot.shape
    scaling = 1.0 / math.sqrt(HEAD_SIZE)
    steps = length // block

    def body(q_ref, kv_ref, o_ref, do_ref, lse_ref, cos_ref, sin_ref, cosf_ref, sinf_ref, posq_ref, posk_ref, dq_ref, dkv_ref, dk_acc, dv_acc):
        @pl.when(pl.program_id(0) == 0)
        def _():
            dk_acc[...] = jnp.zeros_like(dk_acc)
            dv_acc[...] = jnp.zeros_like(dv_acc)

        keys = kv_ref[:, :HEAD_SIZE]
        values = kv_ref[:, HEAD_SIZE : 2 * HEAD_SIZE]
        allowed = posk_ref[...] <= posq_ref[...]
        parts = []
        for h in range(heads):
            at = slice(h * HEAD_SIZE, (h + 1) * HEAD_SIZE)
            q_head = q_ref[:, at]
            grad = do_ref[:, at]
            delta = jnp.sum(grad.astype(F32) * o_ref[:, at].astype(F32), axis=-1, keepdims=True)
            s = lax.dot_general(q_head, keys, LAST_LAST, preferred_element_type=F32) * scaling
            s = jnp.where(allowed, s, NEG_FILL)
            p = jnp.exp(s - lse_ref[:, h : h + 1])
            dp = lax.dot_general(grad, values, LAST_LAST, preferred_element_type=F32)
            ds = (p * (dp - delta)).astype(BF16)
            parts.append(jnp.dot(ds, keys, preferred_element_type=F32) * scaling)
            dk_acc[...] += lax.dot_general(ds, q_head, ROWS_FIRST, preferred_element_type=F32)
            dv_acc[...] += lax.dot_general(p.astype(BF16), grad, ROWS_FIRST, preferred_element_type=F32)
        if heads * HEAD_SIZE < width:
            parts.append(jnp.zeros((block, width - heads * HEAD_SIZE), F32))
        dq = jnp.concatenate(parts, axis=1)
        dq_ref[...] = (dq * cos_ref[...] - swap_halves(dq) * sin_ref[...]).astype(BF16)

        @pl.when(pl.program_id(0) == steps - 1)
        def _():
            dkv = jnp.concatenate([dk_acc[...] * scaling, dv_acc[...]], axis=1)
            lane = lax.broadcasted_iota(jnp.int32, dkv.shape, 1)
            rotated = dkv * cosf_ref[:, : 2 * HEAD_SIZE] - swap_halves(dkv) * sinf_ref[:, : 2 * HEAD_SIZE]
            dkv_ref[...] = jnp.where(lane < HEAD_SIZE, rotated, dkv).astype(BF16)

    row = lambda i: (i, 0)
    whole = lambda i: (0, 0)
    return pl.pallas_call(
        body,
        grid=(steps,),
        out_shape=[
            jax.ShapeDtypeStruct((length, width), BF16),
            jax.ShapeDtypeStruct((length, 2 * HEAD_SIZE), BF16),
        ],
        in_specs=[
            pl.BlockSpec((block, width), row),
            pl.BlockSpec((length, 2 * HEAD_SIZE), whole),
            pl.BlockSpec((block, width), row),
            pl.BlockSpec((block, width), row),
            pl.BlockSpec((block, heads), row),
            pl.BlockSpec((block, width), row),
            pl.BlockSpec((block, width), row),
            pl.BlockSpec((length, cosine.shape[1]), whole),
            pl.BlockSpec((length, cosine.shape[1]), whole),
            pl.BlockSpec((block, 1), row),
            pl.BlockSpec((1, length), whole),
        ],
        out_specs=[
            pl.BlockSpec((block, width), row),
            pl.BlockSpec((length, 2 * HEAD_SIZE), whole),
        ],
        scratch_shapes=[pltpu.VMEM((length, HEAD_SIZE), F32), pltpu.VMEM((length, HEAD_SIZE), F32)],
        name="attend_backward",
        cost_estimate=takes(20),
        compiler_params=pltpu.CompilerParams(vmem_limit_bytes=VMEM_LIMIT),
    )(q_rot, kv_rot, attended, attended_gradient, lse, cosine[:, :width], sine[:, :width], cosine, sine, pos_rows, pos_cols)


def gate_grads(grad_hidden, gate_pre, up_pre):
    sigmoid_gate = jax.nn.sigmoid(gate_pre)
    swish_gate = gate_pre * sigmoid_gate
    grad_gate_pre = (
        grad_hidden * up_pre * sigmoid_gate * (1.0 + gate_pre * (1.0 - sigmoid_gate))
    ).astype(BF16)
    return (grad_gate_pre, (grad_hidden * swish_gate).astype(BF16))


def on_device(
    ndp,
    n,
    block_input,
    piece_order,
    attention_gain,
    query_weight,
    key_matrix,
    value_matrix,
    output_weight,
    feed_gain,
    gate_weight,
    up_weight,
    down_weight,
    cotangent,
):
    _, t, width = block_input.shape
    length = n * t
    rows = query_weight.shape[0]
    heads = QUERY_HEADS // n
    q_width = heads * HEAD_SIZE
    copies = max(1, n // KEY_VALUE_HEADS)
    piece_rows = t // 2

    x_rows = block_input[0]
    grad_rows = cotangent[0]

    offsets = jnp.arange(piece_rows, dtype=jnp.int32)
    pos = ((piece_order * piece_rows)[:, :, None] + offsets[None, None, :]).reshape(-1)
    half = HEAD_SIZE // 2
    frequency = jnp.exp(jnp.arange(half, dtype=F32) * (-2.0 * math.log(ROPE_BASE) / HEAD_SIZE))
    angle = pos.astype(F32)[:, None] * frequency[None, :]
    cos_half, sin_half = jnp.cos(angle), jnp.sin(angle)
    table_heads = max(heads, 2)
    cosine = jnp.tile(jnp.concatenate([cos_half, cos_half], axis=1), (1, table_heads))
    sine = jnp.tile(jnp.concatenate([-sin_half, sin_half], axis=1), (1, table_heads))
    pos_rows, pos_cols = pos[:, None], pos[None, :]
    block = min(256, length)

    def per_head(matrix):
        return jnp.repeat(matrix.reshape(rows, KEY_VALUE_HEADS, HEAD_SIZE), copies, axis=1)

    gains = jnp.stack([attention_gain, feed_gain], axis=1)
    gains = jnp.broadcast_to(jnp.pad(gains, ((0, 0), (0, 126)))[:, None, :], (rows, n, 128))
    kv_gain = jnp.concatenate([per_head(key_matrix), per_head(value_matrix), gains], axis=2)
    kv_gain = kv_gain.reshape(rows, n * 256)
    down_rows = down_weight.T
    q_columns = max(q_width, 128)
    query_columns = query_weight
    if q_columns > q_width:
        query_columns = jnp.pad(
            query_weight.reshape(rows, n, q_width), ((0, 0), (0, 0), (0, q_columns - q_width))
        ).reshape(rows, n * q_columns)

    x_all, w_query, w_kv, w_output, gate_rows = transfer(
        "fetch_first",
        Gather(n, x_rows),
        WeightFetch(n, ndp, query_columns),
        WeightFetch(n, ndp, kv_gain),
        OwnerSpread(n, ndp, output_weight),
        AllToAll(n, gate_weight, True),
    )
    w_output = w_output.reshape(q_width, width)
    gate_cols = lax.all_gather(gate_rows, "dp", axis=0, tiled=True)
    _, grad_rows_later = lax.optimization_barrier((x_all, grad_rows))
    grad_all = lax.all_gather(grad_rows_later, "ctx", axis=0, tiled=True)
    gain_attention = w_kv[:, 128].astype(F32)
    gain_feed = w_kv[:, 129].astype(F32)

    x_all = x_all.reshape(length, width)
    unit_all, _ = normalize(x_all.astype(F32))
    normed_one = (unit_all * gain_attention).astype(BF16)
    query = jnp.dot(normed_one, w_query, preferred_element_type=F32)
    key_value = jnp.dot(normed_one, w_kv, preferred_element_type=F32)
    q_rot, kv_rot, attended, lse = attend_forward(
        query, key_value, cosine, sine, pos_rows, pos_cols, heads, block
    )
    attended = attended[:, :q_width]
    part = jnp.dot(attended, w_output, preferred_element_type=F32).astype(BF16)
    attended_sum, up_rows, down_part = transfer(
        "attended_sum",
        RowSum(n, part.reshape(n, t, width)),
        AllToAll(n, up_weight, True),
        AllToAll(n, down_rows, True),
    )
    grad_all, up_rows, down_part = lax.optimization_barrier((grad_all, up_rows, down_part))
    up_cols, down_cols = (lax.all_gather(w, "dp", axis=0, tiled=True) for w in (up_rows, down_part))
    inputs32 = x_rows.astype(F32)
    unit_one, inv_one = normalize(inputs32)
    mid = inputs32 + attended_sum
    unit_two, inv_two = normalize(mid)
    normed_rows = (unit_two * gain_feed).astype(BF16)
    (normed_all,) = transfer("gather_normed", Gather(n, normed_rows))
    normed_all = normed_all.reshape(length, width)

    gate_pre = jnp.dot(normed_all, gate_cols, preferred_element_type=F32)
    up_pre = jnp.dot(normed_all, up_cols, preferred_element_type=F32)
    hidden = (jax.nn.silu(gate_pre) * up_pre).astype(BF16)
    block_part = lax.dot_general(hidden, down_cols, LAST_LAST, preferred_element_type=F32).astype(BF16)
    block_sum = lax.psum_scatter(block_part, "ctx", scatter_dimension=0, tiled=True)
    _, grad_all = lax.optimization_barrier((block_part, grad_all))
    grad_hidden = jnp.dot(grad_all, down_cols, preferred_element_type=F32)
    grad_gate_pre, grad_up_pre = gate_grads(grad_hidden, gate_pre, up_pre)
    normed_part = (
        lax.dot_general(grad_gate_pre, gate_cols, LAST_LAST, preferred_element_type=F32)
        + lax.dot_general(grad_up_pre, up_cols, LAST_LAST, preferred_element_type=F32)
    ).astype(BF16)
    term_gate = lax.dot_general(normed_all, grad_gate_pre, ROWS_FIRST, preferred_element_type=F32)
    term_up = lax.dot_general(normed_all, grad_up_pre, ROWS_FIRST, preferred_element_type=F32)
    term_down = lax.dot_general(grad_all, hidden, ROWS_FIRST, preferred_element_type=F32)
    terms = tuple(term.astype(BF16) for term in (term_gate, term_up, term_down))
    normed_part, (term_gate, term_up, term_down) = lax.optimization_barrier((normed_part, terms))
    grad_normed_two, gate_sum = transfer(
        "feed_sum", RowSum(n, normed_part.reshape(n, t, width)), DpSum(ndp, term_gate)
    )
    grad_unit_two = grad_normed_two * gain_feed
    grad_mid = grad_rows.astype(F32) + inv_two * (
        grad_unit_two - unit_two * jnp.mean(grad_unit_two * unit_two, axis=-1, keepdims=True)
    )

    grad_mid_all, down_sum, own_gate = transfer(
        "gather_mid", Gather(n, grad_mid.astype(BF16)), DpSum(ndp, term_down), AllToAll(n, gate_sum, False)
    )
    grad_mid_all, block_sum, term_up = lax.optimization_barrier((grad_mid_all, block_sum, term_up))
    up_sum = lax.psum_scatter(term_up, "dp", scatter_dimension=0, tiled=True)
    block_output = (mid + block_sum.astype(F32)).astype(BF16)[None]
    grad_mid_all = grad_mid_all.reshape(length, width)
    attended_gradient = lax.dot_general(
        grad_mid_all, w_output, LAST_LAST, preferred_element_type=F32
    ).astype(BF16)
    term_output = lax.dot_general(attended, grad_mid_all, ROWS_FIRST, preferred_element_type=F32)
    fill = ((0, 0), (0, q_columns - q_width))
    grad_query, grad_kv = attend_backward(
        q_rot, kv_rot, jnp.pad(attended, fill), jnp.pad(attended_gradient, fill), lse, cosine, sine, pos_rows, pos_cols, heads, block
    )
    one_part = (
        lax.dot_general(grad_query, w_query, LAST_LAST, preferred_element_type=F32)
        + lax.dot_general(grad_kv, w_kv[:, :128], LAST_LAST, preferred_element_type=F32)
    ).astype(BF16)
    term_query = lax.dot_general(normed_one, grad_query, ROWS_FIRST, preferred_element_type=F32)
    term_kv = lax.dot_general(normed_one, grad_kv, ROWS_FIRST, preferred_element_type=F32)
    grad_normed_one, own_query, own_kv, own_output, own_up, own_down = transfer(
        "one_sum",
        RowSum(n, one_part.reshape(n, t, width)),
        SumToColumns(n, ndp, term_query.astype(BF16)),
        SumToColumns(n, ndp, term_kv.astype(BF16)),
        SumToOwner(n, ndp, term_output.astype(BF16)),
        AllToAll(n, up_sum, False),
        AllToAll(n, down_sum, False),
    )
    grad_output_w = own_output.astype(F32)
    grad_gate_w, grad_up_w = own_gate.astype(F32), own_up.astype(F32)
    grad_down_w = own_down.astype(F32).T
    grad_query_w = own_query.astype(F32)
    if q_columns > q_width:
        grad_query_w = grad_query_w.reshape(rows, n, q_columns)[:, :, :q_width].reshape(rows, n * q_width)
    columns = jnp.arange(n * 128, dtype=jnp.int32)
    target = columns // 128 // copies * HEAD_SIZE + columns % HEAD_SIZE
    target = target + columns % 128 // HEAD_SIZE * (KEY_VALUE_HEADS * HEAD_SIZE)
    places = jnp.arange(2 * KEY_VALUE_HEADS * HEAD_SIZE, dtype=jnp.int32)
    picks = (target[:, None] == places[None, :]).astype(BF16)
    both = jnp.dot(own_kv, picks, preferred_element_type=F32)
    grad_key_w, grad_value_w = both[:, : KEY_VALUE_HEADS * HEAD_SIZE], both[:, KEY_VALUE_HEADS * HEAD_SIZE :]

    def product(grad, weight):
        return jnp.sum(grad * weight.astype(F32), axis=1)

    grad_attention_w = (
        product(grad_query_w, query_weight)
        + product(grad_key_w, key_matrix)
        + product(grad_value_w, value_matrix)
    ) / attention_gain.astype(F32)
    grad_feed_w = (product(grad_gate_w, gate_weight) + product(grad_up_w, up_weight)) / feed_gain.astype(F32)

    grad_unit_one = grad_normed_one * gain_attention
    input_grad = grad_mid + inv_one * (
        grad_unit_one - unit_one * jnp.mean(grad_unit_one * unit_one, axis=-1, keepdims=True)
    )
    return (
        block_output,
        input_grad.astype(BF16)[None],
        grad_attention_w,
        grad_query_w,
        grad_key_w,
        grad_value_w,
        grad_output_w,
        grad_feed_w,
        grad_gate_w,
        grad_up_w,
        grad_down_w,
    )


def solution(mesh):
    return jax.shard_map(
        functools.partial(on_device, mesh.shape["dp"], mesh.shape["ctx"]),
        mesh=mesh,
        in_specs=(
            P("dp", "ctx", None),
            P(),
            P(("dp", "ctx")),
            P(("dp", "ctx"), None),
            P(("dp", "ctx"), None),
            P(("dp", "ctx"), None),
            P(("dp", "ctx"), None),
            P(("dp", "ctx")),
            P(("dp", "ctx"), None),
            P(("dp", "ctx"), None),
            P(None, ("dp", "ctx")),
            P("dp", "ctx", None),
        ),
        out_specs=(
            P("dp", "ctx", None),
            P("dp", "ctx", None),
            P(("dp", "ctx")),
            P(("dp", "ctx"), None),
            P(("dp", "ctx"), None),
            P(("dp", "ctx"), None),
            P(("dp", "ctx"), None),
            P(("dp", "ctx")),
            P(("dp", "ctx"), None),
            P(("dp", "ctx"), None),
            P(None, ("dp", "ctx")),
        ),
        check_vma=False,
    )
```
